256 devices in a mesh: section: 4 (over y), dp: 64 (over x, z, core).
Axes of the slice: x: 4, y: 4, z: 8, core: 2. Of those that a mesh axis runs over, the one named last changes fastest.
Arguments:
- token_ids: int32 [4, 4096], P(None, 'dp'), may hold values from 0 to 127
- embed: bfloat16 [128, 512], replicated, may hold values from -6 to 6
- weights: bfloat16 [4, 2, 512, 2048], P('section'), may hold values from -0.25 to 0.25
- variance: bfloat16 [4, 1024, 2048], P('section', 'dp'), may hold values from 9.9658966e-05 to 0.0099487305
- momentum: bfloat16 [4, 1024, 2048], P('section', 'dp'), may hold values from -4 to 4
- worker_error: bfloat16 [4, 64, 2, 512, 2048], P('section', 'dp'), may hold values from -6 to 6
- server_error: float32 [4, 1024, 2048], P('section', 'dp'), may hold values from -0.75 to 0.75
- cotangent: bfloat16 [4, 4096, 512], P(None, 'dp'), may hold values from -0.75 to 0.75
Outputs:
- new_weights: bfloat16 [4, 1024, 2048], P('section', 'dp')
- new_momentum: bfloat16 [4, 1024, 2048], P('section', 'dp')
- new_worker_error: bfloat16 [4, 64, 2, 512, 2048], P('section', 'dp')
- new_server_error: float32 [4, 1024, 2048], P('section', 'dp')
The draws below stay inside these ranges and needn't reach their ends.
All inputs are finite; a program needn't handle non-finite values.
Results may differ from the reference program's by a relative error of at most 0.012.
Values may be sent and summed in bfloat16 or wider, within the bound.
A program may use at most 128 MiB of HBM per device.

```python
import math
import jax
import jax.numpy as jnp
import numpy as np
from jax import lax

D = 512
HC = 2048
VW = 128
MB = 4
TOK_MB = 64
TOKENS = 4096
N_SECTION = 4
N_DP = 64


def with_ends(entries, own_key, least, high):
    longest = entries.shape.index(max(entries.shape))
    spots = []
    for shift in (0, 1):
        where = [jax.random.randint(jax.random.fold_in(own_key, axis), (), 0, length) for axis, length in enumerate(entries.shape)]
        where[longest] = (where[longest] + shift) % entries.shape[longest]
        spots.append(tuple(where))
    return entries.at[spots[0]].set(least).at[spots[1]].set(high)


def with_spikes(values, stream_key, source, target, blocks, factor):
    owner, partner = [(jnp.arange(values.shape[dim]) // (values.shape[dim] // blocks)).reshape([-1 if axis == dim else 1 for axis in range(values.ndim)]) for dim in (source, target)]
    chosen = jax.random.permutation(stream_key, blocks)[partner]
    strong = (owner == chosen) | (owner == (partner + blocks // 2) % blocks)
    return jnp.where(strong, factor * values, values)


def block_scale(own_key, shape, shards, smallest, largest):
    level = 1.0
    for axis_at, parts in shards:
        draws = jax.random.uniform(jax.random.fold_in(jax.random.fold_in(own_key, 6), axis_at), (parts,), jnp.float32, smallest / len(shards), largest / len(shards))
        level = level * jnp.repeat(jnp.exp(draws), shape[axis_at] // parts).reshape((-1,) + (1,) * (len(shape) - 1 - axis_at))
    return level


def rank_table(number_of, slope):
    weights = [(1 << 20) // math.isqrt(standing ** slope) + 1 for standing in range(1, number_of + 1)]
    width = 1 + sum(weights) // (1 << 30)
    return np.cumsum(np.array([max(1, weight // width) for weight in weights]))


def skewed_ids(own_key, extent, count, slope):
    table = rank_table(count, slope)
    pick = jax.random.randint(jax.random.fold_in(own_key, 1), extent, 0, int(table[count - 1]))
    standing = jnp.searchsorted(jnp.asarray(table, jnp.int32), pick, side="right")
    return jax.random.permutation(jax.random.fold_in(own_key, 2), count)[standing].astype(jnp.int32)


def centred(key, shape, width, limit, shards=(), kind=jnp.bfloat16):
    values = width * jax.random.normal(key, shape, jnp.float32)
    if shards:
        values = values * block_scale(key, shape, shards, -0.22, 0.18)
    return jnp.clip(values, -limit, limit).astype(kind)


def heavy_noise(rng, dims, deviation, reach, shards, heavy, kind=jnp.bfloat16):
    result = deviation * jax.random.normal(rng, dims, jnp.float32)
    if shards:
        result = result * block_scale(rng, dims, shards, -0.22, 0.18)
    return jnp.clip(with_spikes(result, jax.random.fold_in(rng, 3), *heavy), -reach, reach).astype(kind)


def setup_inputs(seed: int = 0) -> dict:
    splits = jax.random.split(jax.random.key(seed), 9)
    token_ids = with_ends(skewed_ids(splits[0], (MB, TOKENS), VW, 2), jax.random.fold_in(splits[0], 3), 0, VW - 1).astype(jnp.int32)
    embed = centred(splits[1], (VW, D), 1.0, 6.0)
    weights = centred(splits[2], (N_SECTION, 2, D, HC), D ** -0.5, 0.25, ((0, 4),))
    variance = jnp.clip(jnp.exp(math.log(0.0099487305) - 4.603446 * jax.random.uniform(splits[3], (N_SECTION, 2 * D, HC), jnp.float32) ** block_scale(splits[3], (N_SECTION, 2 * D, HC), ((0, 4), (1, 64)), -0.2, 0.2)), 9.965896606445312e-05, 0.0099487305).astype(jnp.bfloat16)
    momentum = centred(splits[4], (N_SECTION, 2 * D, HC), 0.5, 4.0, ((0, 4), (1, 64)))
    worker_error = heavy_noise(splits[5], (N_SECTION, N_DP, 2, D, HC), 0.3, 6.0, ((0, 4), (1, 64)), (1, 3, 64, 4.0))
    server_error = centred(splits[6], (N_SECTION, 2 * D, HC), 0.05, 0.75, ((0, 4), (1, 64)), jnp.float32)
    cotangent = centred(splits[7], (MB, TOKENS, D), 0.05, 0.75, ((1, 64),))
    return dict(token_ids=token_ids, embed=embed, weights=weights, variance=variance, momentum=momentum, worker_error=worker_error, server_error=server_error, cotangent=cotangent)


gelu_coef = math.sqrt(2.0 / math.pi)

def gelu_value(upper):
    inner = gelu_coef * (upper + 0.044715 * upper * upper * upper)
    return 0.5 * upper * (1.0 + jnp.tanh(inner))

def gelu_slope(upper):
    inner = gelu_coef * (upper + 0.044715 * upper * upper * upper)
    bent = jnp.tanh(inner)
    return 0.5 * (1.0 + bent) + 0.5 * upper * (1.0 - bent * bent) * gelu_coef * (1.0 + 3.0 * 0.044715 * upper * upper)

def normalize(inputs):
    values = inputs.astype(jnp.float32)
    center = lax.optimization_barrier(jnp.mean(values, axis=-1, keepdims=True))
    spread = lax.optimization_barrier(jnp.mean((values - center) * (values - center), axis=-1, keepdims=True))
    scaled = lax.rsqrt(spread + 1e-05)
    return ((values - center) * scaled, scaled)

def forward_block(inputs, first_matrix, second_matrix):
    normed, scaled = normalize(inputs)
    normed_b = normed.astype(jnp.bfloat16)
    upper = jnp.dot(normed_b, first_matrix, preferred_element_type=jnp.float32)
    hidden = gelu_value(upper).astype(jnp.bfloat16)
    mixed = lax.dot_general(hidden, second_matrix, (((1,), (1,)), ((), ())), preferred_element_type=jnp.float32)
    output = (inputs.astype(jnp.float32) + mixed).astype(jnp.bfloat16)
    return (output, normed, scaled, normed_b, upper, hidden)

def backward_block(grad_out, normed, scaled, upper, first_matrix, second_matrix):
    back_hidden = jnp.dot(grad_out, second_matrix, preferred_element_type=jnp.float32)
    back_upper = (back_hidden * gelu_slope(upper)).astype(jnp.bfloat16)
    back_normed = lax.dot_general(back_upper, first_matrix, (((1,), (1,)), ((), ())), preferred_element_type=jnp.float32)
    first_mean = lax.optimization_barrier(jnp.mean(back_normed, axis=-1, keepdims=True))
    second_mean = lax.optimization_barrier(jnp.mean(back_normed * normed, axis=-1, keepdims=True))
    grad_in = (grad_out.astype(jnp.float32) + scaled * (back_normed - first_mean - normed * second_mean)).astype(jnp.bfloat16)
    return (grad_in, back_upper)

def replica_sum(left, right):
    left_rows = left.astype(jnp.float32).reshape(MB, N_DP, TOK_MB, left.shape[-1])
    right_rows = right.astype(jnp.float32).reshape(MB, N_DP, TOK_MB, right.shape[-1])
    return jnp.einsum('mrtd,mrth->rdh', left_rows, right_rows, precision=lax.Precision.HIGHEST)

def reference(token_ids, embed, weights, variance, momentum, worker_error, server_error, cotangent):
    state = jnp.take(embed, token_ids.reshape(-1).astype(jnp.int32), axis=0)
    saved = []
    for section in range(N_SECTION):
        output, normed, scaled, normed_b, upper, hidden = forward_block(state, weights[section, 0], weights[section, 1])
        saved.append((normed, scaled, normed_b, upper, hidden))
        state = output
    grad = cotangent.reshape(-1, D)
    results = [None] * N_SECTION
    for section in range(N_SECTION - 1, -1, -1):
        normed, scaled, normed_b, upper, hidden = saved[section]
        grad_in, back_upper = backward_block(grad, normed, scaled, upper, weights[section, 0], weights[section, 1])
        gradient = jnp.stack([replica_sum(normed_b, back_upper), replica_sum(grad, hidden)], axis=1)
        shared = momentum[section].astype(jnp.float32).reshape(2, D, HC)
        combined = 0.9 * shared[None] + 0.1 * gradient + worker_error[section].astype(jnp.float32)
        worker_scale = jnp.sqrt(lax.optimization_barrier(jnp.mean(combined * combined, axis=(1, 2, 3), keepdims=True)) + 0.01)
        packed = (worker_scale * jnp.tanh(combined / worker_scale)).astype(jnp.bfloat16)
        fresh_worker = (combined - packed.astype(jnp.float32)).astype(jnp.bfloat16)
        merged = (lax.optimization_barrier(jnp.sum(packed.astype(jnp.float32), axis=0)) / N_DP).reshape(2 * D, HC) + server_error[section]
        blocks = merged.reshape(N_DP, -1)
        server_scale = jnp.sqrt(lax.optimization_barrier(jnp.mean(blocks * blocks, axis=1, keepdims=True)) + 0.01)
        server_values = (server_scale * jnp.tanh(blocks / server_scale)).astype(jnp.bfloat16)
        fresh_server = (blocks - server_values.astype(jnp.float32)).reshape(2 * D, HC)
        averaged = server_values.reshape(2 * D, HC)
        step_size = 0.01 * averaged.astype(jnp.float32) / (jnp.sqrt(variance[section].astype(jnp.float32)) + 1e-08)
        fresh_weights = (weights[section].astype(jnp.float32).reshape(2 * D, HC) - step_size).astype(jnp.bfloat16)
        results[section] = (fresh_weights, averaged, fresh_worker, fresh_server)
        grad = grad_in
    new_weights = jnp.stack([item[0] for item in results])
    new_momentum = jnp.stack([item[1] for item in results])
    new_worker_error = jnp.stack([item[2] for item in results])
    new_server_error = jnp.stack([item[3] for item in results])
    return (new_weights, new_momentum, new_worker_error, new_server_error)
```

```python
import functools
import math

import jax
import jax.numpy as jnp
from jax import lax
from jax.experimental import pallas as pl
from jax.experimental.pallas import tpu as pltpu
from jax.sharding import PartitionSpec as P

gelu_coef = math.sqrt(2.0 / math.pi)
MESH = pl.DeviceIdType.MESH
BF = jnp.bfloat16
F32 = jnp.float32
NX = 4
NC = 2


def dot_nn(a, b):
    return lax.dot_general(a, b, (((1,), (0,)), ((), ())), preferred_element_type=F32)


def dot_nt(a, b):
    return lax.dot_general(a, b, (((1,), (1,)), ((), ())), preferred_element_type=F32)


def dot_tn(a, b):
    return lax.dot_general(a, b, (((0,), (0,)), ((), ())), preferred_element_type=F32)


def step_kernel(
    ns, nz, mb, tok, d, hc, tile,
    ids_ref, embed_ref, w_hbm, var_ref, mom_hbm, we_hbm, se_ref, cot_ref,
    nw_ref, nm_ref, ne_hbm, nse_ref,
    w, own_w, we, mom, comb, packed, ne, xin, fout, gout, nf, scf, slope, left, right,
    d0, s0, ra, fa, fb, s1, zr,
    loc, f_s, f_r, b_s, b_r, gz_s, gz_r, gx_s, gx_r, gd_s, gd_r,
    d_s, d_r, a_s, a_r, ta_s, ta_r, tb_s, tb_r, z_s, z_r,
):
    s = lax.axis_index("section")
    r = lax.axis_index("dp")
    core = r % NC
    z = (r // NC) % nz
    x = r // (NC * nz)
    na = x + 1 - 2 * (x % 2)
    nb = 3 - x
    opp = (x + 2) % 4
    half = nz // 2
    ng = nz // 4

    def at(xx, zz, cc):
        return (xx * nz + zz) * NC + cc

    partner = at(x, z, 1 - core)
    dev_a = at(na, z, core)
    dev_b = at(nb, z, core)

    def dev_z(zeta):
        return at(x, (z + zeta) % nz, core)

    def remote(src, dst, send, recv, to):
        return pltpu.make_async_remote_copy(
            src_ref=src, dst_ref=dst, send_sem=send, recv_sem=recv,
            device_id={"dp": to}, device_id_type=MESH,
        )

    barrier = pltpu.get_barrier_semaphore()
    for peer in [partner, dev_a, dev_b] + [dev_z(k) for k in range(1, nz)]:
        pl.semaphore_signal(barrier, inc=1, device_id={"dp": peer}, device_id_type=MESH)

    @pl.when(s > 0)
    def _():
        pl.semaphore_signal(barrier, inc=1, device_id={"section": s - 1}, device_id_type=MESH)

    @pl.when(s < ns - 1)
    def _():
        pl.semaphore_signal(barrier, inc=1, device_id={"section": s + 1}, device_id_type=MESH)

    cp_mom = pltpu.make_async_copy(mom_hbm.at[0], mom.at[x, z, core], loc.at[0])
    cp_w0 = pltpu.make_async_copy(w_hbm.at[0, 0], w.at[0], loc.at[1])
    cp_w1 = pltpu.make_async_copy(w_hbm.at[0, 1], w.at[1], loc.at[2])
    cp_we = pltpu.make_async_copy(we_hbm, we, loc.at[3])
    cp_ow = pltpu.make_async_copy(
        w_hbm.at[0, x // 2, pl.ds(pl.multiple_of((r % (NC * nz * 2)) * 16, 16), 16)], own_w, loc.at[4]
    )
    cp_mom.start()
    cp_w0.start()
    cp_w1.start()
    cp_ow.start()
    cp_we.start()

    @pl.when(s == 0)
    def _():
        vocab = embed_ref.shape[0]
        for m in range(mb):
            hot = (
                lax.broadcasted_iota(jnp.int32, (vocab, tok), 0) == ids_ref[m : m + 1, :]
            ).astype(F32).astype(BF)
            xin[m] = dot_tn(hot, embed_ref[...]).astype(BF)

    @pl.when(s == ns - 1)
    def _():
        left[1] = cot_ref[...]

    pl.semaphore_wait(
        barrier, 2 + nz + jnp.where(s > 0, 1, 0) + jnp.where(s < ns - 1, 1, 0)
    )

    cp_mom.wait()

    def g_z(zeta):
        blk = mom.at[x, z, core]
        return remote(blk, blk, gz_s.at[zeta - 1], gz_r.at[zeta - 1], dev_z(zeta))

    def g_z_in(zeta):
        blk = mom.at[x, (z + nz - zeta) % nz, core]
        return remote(blk, blk, gz_s.at[zeta - 1], gz_r.at[zeta - 1], dev_z(zeta))

    def g_x(xx, lo, n, k, to):
        blk = mom.at[xx, pl.ds(lo, n), core]
        return remote(blk, blk, gx_s.at[k], gx_r.at[k], to)

    def g_d(xx, cc, k):
        blk = mom.at[xx, pl.ds(0, nz), cc]
        return remote(blk, blk, gd_s.at[k], gd_r.at[k], partner)

    for k in range(nz):
        zeta = half + k // 2 if k % 2 == 0 else half - 1 - k // 2
        if zeta:
            g_z(zeta).start()

    cp_w0.wait()
    cp_w1.wait()

    def send_f(m):
        return pltpu.make_async_remote_copy(
            src_ref=fout.at[m], dst_ref=xin.at[m], send_sem=f_s.at[m], recv_sem=f_r.at[m],
            device_id={"section": jnp.minimum(s + 1, ns - 1)}, device_id_type=MESH,
        )

    def send_b(m):
        return pltpu.make_async_remote_copy(
            src_ref=gout.at[m], dst_ref=left.at[1, m], send_sem=b_s.at[m], recv_sem=b_r.at[m],
            device_id={"section": jnp.maximum(s - 1, 0)}, device_id_type=MESH,
        )

    nt = hc // tile

    @pl.loop(0, 2 * (ns - 1) + mb)
    def _(t):
        mf = t - s
        mbk = t - (2 * (ns - 1) - s)

        @pl.when(t == 4 + jnp.where(s == 1, 1, 0))
        def _():
            for zeta in range(1, nz):
                g_z_in(zeta).wait_recv()
            g_x(x, 0, nz, 0, dev_a).start()
            g_x(x, 0, nz, 1, dev_b).start()
            g_d(x, core, 0).start()

        @pl.when(t == 5 + (s + 1) // 2)
        def _():
            g_x(na, 0, nz, 0, dev_a).wait_recv()
            g_x(nb, 0, nz, 1, dev_b).wait_recv()
            g_x(nb, 0, half, 2, dev_a).start()
            g_x(na, half, half, 3, dev_b).start()
            g_d(na, core, 1).start()
            g_d(nb, core, 2).start()

        @pl.when(t == 2 * (ns - 1) + mb - 1)
        def _():
            g_x(opp, 0, half, 2, dev_a).wait_recv()
            g_x(opp, half, half, 3, dev_b).wait_recv()
            g_d(opp, core, 3).start()

        @pl.when(jnp.logical_and(mf >= 0, mf < mb))
        def _():
            @pl.when(s > 0)
            def _():
                send_f(mf).wait_recv()

            xv = xin[mf].astype(F32)
            center = jnp.mean(xv, axis=-1, keepdims=True)
            dev = xv - center
            spread = jnp.mean(dev * dev, axis=-1, keepdims=True)
            scaled = lax.rsqrt(spread + 1e-05)
            normed = dev * scaled
            nf[mf] = normed
            scf[mf] = jnp.broadcast_to(scaled, (tok, 128))
            nbv = normed.astype(BF)
            left[0, mf] = nbv
            acc = xv
            for j in range(nt):
                cols = slice(j * tile, (j + 1) * tile)
                u = dot_nn(nbv, w[0, :, cols])
                uu = u * u
                bent = jnp.tanh(u * (gelu_coef + (gelu_coef * 0.044715) * uu))
                hu = 0.5 * u
                hp = 0.5 + 0.5 * bent
                hid = (u * hp).astype(BF)
                right[1, mf, :, cols] = hid
                slope[mf, :, cols] = hp + hu * (1.0 - bent * bent) * (
                    gelu_coef + (gelu_coef * 3.0 * 0.044715) * uu
                )
                acc = acc + dot_nt(hid, w[1, :, cols])

            @pl.when(s < ns - 1)
            def _():
                fout[mf] = acc.astype(BF)
                send_f(mf).start()

        @pl.when(jnp.logical_and(mbk >= 0, mbk < mb))
        def _():
            @pl.when(s < ns - 1)
            def _():
                send_b(mbk).wait_recv()

            g = left[1, mbk]
            for j in range(nt):
                cols = slice(j * tile, (j + 1) * tile)
                bh = dot_nn(g, w[1, :, cols])
                right[0, mbk, :, cols] = (bh * slope[mbk, :, cols]).astype(BF)

            @pl.when(s > 0)
            def _():
                bn = dot_nt(right[0, mbk], w[0])
                normed = nf[mbk]
                first = jnp.mean(bn, axis=-1, keepdims=True)
                second = jnp.mean(bn * normed, axis=-1, keepdims=True)
                sc = scf[mbk][:, :1]
                gout[mbk] = (g.astype(F32) + sc * (bn - first - normed * second)).astype(BF)
                send_b(mbk).start()

    cp_we.wait()
    for k, xx in enumerate((x, na, nb, opp)):
        g_d(xx, 1 - core, k).wait_recv()

    qx = NX // 2
    ct = 512 if hc % 512 == 0 else 256
    nct = hc // ct
    rows = qx * nz * NC * 16

    def first_pass(idx, sq):
        i = idx // nct
        j = pl.multiple_of((idx % nct) * ct, ct)
        lt = left[i].reshape(mb * tok, d)
        rt = right[i, :, :, pl.ds(j, ct)].reshape(mb * tok, ct)
        grad = dot_tn(lt, rt)
        shared = mom[pl.ds(i * qx, qx), :, :, :, pl.ds(j, ct)].reshape(rows, ct).astype(F32)
        err = we[pl.ds(i * qx, qx), :, :, :, pl.ds(j, ct)].reshape(rows, ct).astype(F32)
        c = 0.9 * shared + 0.1 * grad + err
        comb[pl.ds(i * qx, qx), :, :, :, pl.ds(j, ct)] = c.reshape(qx, nz, NC, 16, ct)
        return sq + jnp.sum((c * c).reshape(rows // 8, 8, ct), axis=0)

    sq = lax.fori_loop(0, 2 * nct, first_pass, jnp.zeros((8, ct), F32))
    total_sq = jnp.sum(jnp.sum(sq, axis=0, keepdims=True), axis=1, keepdims=True)
    scale = jnp.sqrt(total_sq * (1.0 / (2 * d * hc)) + 0.01)
    inverse = 1.0 / scale

    def second_pass(q):
        @pl.loop(0, nz)
        def _(k):
            c = comb[q, k].reshape(NC * 16, hc)
            p = (scale * jnp.tanh(c * inverse)).astype(BF)
            packed[q, k] = p.reshape(NC, 16, hc)
            ne[q, k] = (c - p.astype(F32)).astype(BF).reshape(NC, 16, hc)

    def cp_ne(q, k):
        return pltpu.make_async_copy(ne.at[q], ne_hbm.at[q], loc.at[5 + k])

    def to_partner(q, k):
        return remote(packed.at[q, pl.ds(0, nz), 1 - core], d0.at[k], d_s.at[k], d_r.at[k], partner)

    def pair_sum(q, k):
        to_partner(q, k).wait_recv()

        @pl.loop(0, nz)
        def _(i):
            zeta = half + i // 2 - (i % 2) * (1 + 2 * (i // 2))
            zz = (z + zeta) % nz
            s0[k, i] = (packed[q, zz, core].astype(F32) + d0[k, zz].astype(F32)).astype(BF)

    def grp(ref, g):
        return ref.at[pl.ds(g * ng, ng)]

    def send_opp(g):
        to = dev_a if g % 2 == 0 else dev_b
        return remote(grp(s0.at[0], g), grp(ra, g), a_s.at[g], a_r.at[g], to)

    def send_a(g):
        return remote(grp(s0.at[1], g), grp(fa, g), ta_s.at[g], ta_r.at[g], dev_a)

    def send_bb(g):
        return remote(grp(s0.at[2], g), grp(fb, g), tb_s.at[g], tb_r.at[g], dev_b)

    def augment(g):
        send_opp(g).wait_recv()
        slot = 2 if g % 2 == 0 else 1

        @pl.loop(0, ng)
        def _(i):
            k = g * ng + i
            s0[slot, k] = (s0[slot, k].astype(F32) + ra[k].astype(F32)).astype(BF)

        (send_bb if slot == 2 else send_a)(g).start()

    def z_of(k):
        return half + k // 2 if k % 2 == 0 else half - 1 - k // 2

    def send_z(k):
        return remote(s1.at[k], zr.at[k], z_s.at[k], z_r.at[k], dev_z(z_of(k)))

    def along_z(groups):
        for g in groups:
            send_a(g).wait_recv()
            send_bb(g).wait_recv()
            for i in range(ng):
                k = g * ng + i
                s1[k] = (s0[3, k].astype(F32) + fa[k].astype(F32) + fb[k].astype(F32)).astype(BF)
                if z_of(k):
                    send_z(k).start()

    second_pass(opp)
    to_partner(opp, 0).start()
    cp_ne(opp, 0).start()
    second_pass(na)
    to_partner(na, 1).start()
    cp_ne(na, 1).start()
    pair_sum(opp, 0)
    send_opp(0).start()
    send_opp(1).start()
    second_pass(nb)
    to_partner(nb, 2).start()
    cp_ne(nb, 2).start()
    pair_sum(na, 1)
    send_a(0).start()
    second_pass(x)
    to_partner(x, 3).start()
    cp_ne(x, 3).start()
    pair_sum(nb, 2)
    send_bb(1).start()
    send_opp(2).start()
    send_opp(3).start()
    augment(0)
    augment(1)
    send_a(2).start()
    send_bb(3).start()
    pair_sum(x, 3)
    augment(2)
    augment(3)
    along_z((0, 1))
    along_z((2, 3))

    total = s1[nz - 1].astype(F32)
    for k in range(nz - 1):
        send_z(k).wait_recv()
        total = total + zr[k].astype(F32)
    merged = total * (1.0 / (NX * nz * NC)) + se_ref[0]
    msq = jnp.sum(jnp.sum(merged * merged, axis=0, keepdims=True), axis=1, keepdims=True)
    sscale = jnp.sqrt(msq * (1.0 / (16 * hc)) + 0.01)
    values = (sscale * jnp.tanh(merged * (1.0 / sscale))).astype(BF)
    vf = values.astype(F32)
    nm_ref[0] = values
    nse_ref[0] = merged - vf
    cp_ow.wait()
    step = 0.01 * vf / (jnp.sqrt(var_ref[0].astype(F32)) + 1e-08)
    nw_ref[0] = (own_w[...].astype(F32) - step).astype(BF)

    for m in range(mb):
        @pl.when(s < ns - 1)
        def _():
            send_f(m).wait_send()

        @pl.when(s > 0)
        def _():
            send_b(m).wait_send()

    for zeta in range(1, nz):
        g_z(zeta).wait_send()
    g_x(x, 0, nz, 0, dev_a).wait_send()
    g_x(x, 0, nz, 1, dev_b).wait_send()
    g_x(nb, 0, half, 2, dev_a).wait_send()
    g_x(na, half, half, 3, dev_b).wait_send()
    for k, xx in enumerate((x, na, nb, opp)):
        g_d(xx, core, k).wait_send()
    for k, q in enumerate((opp, na, nb, x)):
        to_partner(q, k).wait_send()
        cp_ne(q, k).wait()
    for g in range(4):
        send_opp(g).wait_send()
        send_a(g).wait_send()
        send_bb(g).wait_send()
    for k in range(nz - 1):
        send_z(k).wait_send()


def local(ns, nz, token_ids, embed, weights, variance, momentum, worker_error, server_error, cotangent):
    mb, tok = token_ids.shape
    d = embed.shape[1]
    hc = weights.shape[3]
    dims = (NX, nz, NC, 16, hc)
    vm = pl.BlockSpec(memory_space=pltpu.VMEM)
    hbm = pl.BlockSpec(memory_space=pl.ANY)
    dma = pltpu.SemaphoreType.DMA
    tile = 512 if hc % 512 == 0 else 128
    kernel = functools.partial(step_kernel, ns, nz, mb, tok, d, hc, tile)
    nw, nm, ne, nse = pl.pallas_call(
        kernel,
        out_shape=(
            jax.ShapeDtypeStruct((1, 16, hc), BF),
            jax.ShapeDtypeStruct((1, 16, hc), BF),
            jax.ShapeDtypeStruct(dims, BF),
            jax.ShapeDtypeStruct((1, 16, hc), F32),
        ),
        in_specs=[vm, vm, hbm, vm, hbm, hbm, vm, vm],
        out_specs=(vm, vm, hbm, vm),
        scratch_shapes=[
            pltpu.VMEM((2, d, hc), BF),
            pltpu.VMEM((16, hc), BF),
            pltpu.VMEM(dims, BF),
            pltpu.VMEM(dims, BF),
            pltpu.VMEM(dims, F32),
            pltpu.VMEM(dims, BF),
            pltpu.VMEM(dims, BF),
            pltpu.VMEM((mb, tok, d), BF),
            pltpu.VMEM((mb, tok, d), BF),
            pltpu.VMEM((mb, tok, d), BF),
            pltpu.VMEM((mb, tok, d), F32),
            pltpu.VMEM((mb, tok, 128), F32),
            pltpu.VMEM((mb, tok, hc), F32),
            pltpu.VMEM((2, mb, tok, d), BF),
            pltpu.VMEM((2, mb, tok, hc), BF),
            pltpu.VMEM((4, nz, 16, hc), BF),
            pltpu.VMEM((4, nz, 16, hc), BF),
            pltpu.VMEM((nz, 16, hc), BF),
            pltpu.VMEM((nz, 16, hc), BF),
            pltpu.VMEM((nz, 16, hc), BF),
            pltpu.VMEM((nz, 16, hc), BF),
            pltpu.VMEM((nz, 16, hc), BF),
            dma((9,)),
            dma((mb,)), dma((mb,)), dma((mb,)), dma((mb,)),
            dma((nz - 1,)), dma((nz - 1,)), dma((4,)), dma((4,)), dma((4,)), dma((4,)),
            dma((4,)), dma((4,)), dma((4,)), dma((4,)), dma((4,)), dma((4,)), dma((4,)), dma((4,)),
            dma((nz,)), dma((nz,)),
        ],
        compiler_params=pltpu.CompilerParams(
            collective_id=0, has_side_effects=True, vmem_limit_bytes=60 * 1024 * 1024
        ),
        name="step",
    )(
        token_ids, embed, weights, variance, momentum,
        worker_error.reshape(dims), server_error, cotangent,
    )
    return (nw, nm, ne.reshape(worker_error.shape), nse)


def solution(mesh):
    ns = mesh.shape["section"]
    nz = mesh.shape["dp"] // (NX * NC)
    in_specs = (
        P(None, "dp"),
        P(),
        P("section", None, None, None),
        P("section", "dp", None),
        P("section", "dp", None),
        P("section", "dp", None, None, None),
        P("section", "dp", None),
        P(None, "dp", None),
    )
    out_specs = (
        P("section", "dp", None),
        P("section", "dp", None),
        P("section", "dp", None, None, None),
        P("section", "dp", None),
    )
    return jax.shard_map(
        functools.partial(local, ns, nz), mesh=mesh, in_specs=in_specs, out_specs=out_specs,
        check_vma=False,
    )
```

```python
import functools
import math

import jax
import jax.numpy as jnp
from jax import lax
from jax.experimental import pallas as pl
from jax.experimental.pallas import tpu as pltpu
from jax.sharding import PartitionSpec as P

gelu_coef = math.sqrt(2.0 / math.pi)
MESH = pl.DeviceIdType.MESH
BF = jnp.bfloat16
F32 = jnp.float32
NX = 4
NC = 2


def dot_nn(a, b):
    return lax.dot_general(a, b, (((1,), (0,)), ((), ())), preferred_element_type=F32)


def dot_nt(a, b):
    return lax.dot_general(a, b, (((1,), (1,)), ((), ())), preferred_element_type=F32)


def dot_tn(a, b):
    return lax.dot_general(a, b, (((0,), (0,)), ((), ())), preferred_element_type=F32)


def step_kernel(
    ns, nz, mb, tok, d, hc, tile,
    ids_hbm, embed_hbm, w_hbm, var_hbm, mom_hbm, we_hbm, se_hbm, cot_hbm,
    nw_ref, nm_ref, ne, nse_ref,
    ids, embed, var, se, w, own_w, we, mom, comb, packed, xin, fout, gout, nf, scf, slope, left, right,
    d0, s0, ra, fa, fb, s1, zr,
    loc, f_s, f_r, b_s, b_r, gz_s, gz_r, gx_s, gx_r, gd_s, gd_r,
    d_s, d_r, a_s, a_r, ta_s, ta_r, tb_s, tb_r, z_s, z_r,
):
    s = lax.axis_index("section")
    r = lax.axis_index("dp")
    core = r % NC
    z = (r // NC) % nz
    x = r // (NC * nz)
    na = x + 1 - 2 * (x % 2)
    nb = 3 - x
    opp = (x + 2) % 4
    half = nz // 2
    ng = nz // 4

    def at(xx, zz, cc):
        return (xx * nz + zz) * NC + cc

    partner = at(x, z, 1 - core)
    dev_a = at(na, z, core)
    dev_b = at(nb, z, core)

    def dev_z(zeta):
        return at(x, (z + zeta) % nz, core)

    def remote(src, dst, send, recv, to):
        return pltpu.make_async_remote_copy(
            src_ref=src, dst_ref=dst, send_sem=send, recv_sem=recv,
            device_id={"dp": to}, device_id_type=MESH,
        )

    barrier = pltpu.get_barrier_semaphore()
    for peer in [partner, dev_a, dev_b] + [dev_z(k) for k in range(1, nz)]:
        pl.semaphore_signal(barrier, inc=1, device_id={"dp": peer}, device_id_type=MESH)

    @pl.when(s > 0)
    def _():
        pl.semaphore_signal(barrier, inc=1, device_id={"section": s - 1}, device_id_type=MESH)

    @pl.when(s < ns - 1)
    def _():
        pl.semaphore_signal(barrier, inc=1, device_id={"section": s + 1}, device_id_type=MESH)

    cp_mom = pltpu.make_async_copy(mom_hbm.at[0], mom.at[x, z, core], loc.at[0])
    cp_w0 = pltpu.make_async_copy(w_hbm.at[0, 0], w.at[0], loc.at[1])
    cp_w1 = pltpu.make_async_copy(w_hbm.at[0, 1], w.at[1], loc.at[2])
    cp_we = pltpu.make_async_copy(we_hbm, we, loc.at[3])
    cp_ow = pltpu.make_async_copy(
        w_hbm.at[0, x // 2, pl.ds(pl.multiple_of((r % (NC * nz * 2)) * 16, 16), 16)], own_w, loc.at[4]
    )
    cp_ids = pltpu.make_async_copy(ids_hbm, ids, loc.at[5])
    cp_embed = pltpu.make_async_copy(embed_hbm, embed, loc.at[6])
    cp_var = pltpu.make_async_copy(var_hbm, var, loc.at[7])
    cp_se = pltpu.make_async_copy(se_hbm, se, loc.at[8])
    cp_cot = pltpu.make_async_copy(cot_hbm, left.at[1], loc.at[9])
    cp_mom.start()

    @pl.when(s == 0)
    def _():
        cp_ids.start()
        cp_embed.start()

    cp_w0.start()
    cp_w1.start()

    @pl.when(s == ns - 1)
    def _():
        cp_cot.start()

    cp_we.start()
    cp_ow.start()
    cp_var.start()
    cp_se.start()

    @pl.when(s == 0)
    def _():
        vocab = embed.shape[0]
        cp_ids.wait()
        cp_embed.wait()
        for m in range(mb):
            hot = (
                lax.broadcasted_iota(jnp.int32, (vocab, tok), 0) == ids[m : m + 1, :]
            ).astype(F32).astype(BF)
            xin[m] = dot_tn(hot, embed[...]).astype(BF)

    @pl.when(s == ns - 1)
    def _():
        cp_cot.wait()

    pl.semaphore_wait(
        barrier, 2 + nz + jnp.where(s > 0, 1, 0) + jnp.where(s < ns - 1, 1, 0)
    )

    cp_mom.wait()

    def g_z(zeta):
        blk = mom.at[x, z, core]
        return remote(blk, blk, gz_s.at[zeta - 1], gz_r.at[zeta - 1], dev_z(zeta))

    def g_z_in(zeta):
        blk = mom.at[x, (z + nz - zeta) % nz, core]
        return remote(blk, blk, gz_s.at[zeta - 1], gz_r.at[zeta - 1], dev_z(zeta))

    def g_x(xx, lo, n, k, to):
        blk = mom.at[xx, pl.ds(lo, n), core]
        return remote(blk, blk, gx_s.at[k], gx_r.at[k], to)

    def g_d(xx, cc, k):
        blk = mom.at[xx, pl.ds(0, nz), cc]
        return remote(blk, blk, gd_s.at[k], gd_r.at[k], partner)

    for k in range(nz):
        zeta = half + k // 2 if k % 2 == 0 else half - 1 - k // 2
        if zeta:
            g_z(zeta).start()

    cp_w0.wait()
    cp_w1.wait()

    def send_f(m):
        return pltpu.make_async_remote_copy(
            src_ref=fout.at[m], dst_ref=xin.at[m], send_sem=f_s.at[m], recv_sem=f_r.at[m],
            device_id={"section": jnp.minimum(s + 1, ns - 1)}, device_id_type=MESH,
        )

    def send_b(m):
        return pltpu.make_async_remote_copy(
            src_ref=gout.at[m], dst_ref=left.at[1, m], send_sem=b_s.at[m], recv_sem=b_r.at[m],
            device_id={"section": jnp.maximum(s - 1, 0)}, device_id_type=MESH,
        )

    nt = hc // tile

    @pl.loop(0, 2 * (ns - 1) + mb)
    def _(t):
        mf = t - s
        mbk = t - (2 * (ns - 1) - s)

        @pl.when(t == 4 + jnp.where(s == 1, 1, 0))
        def _():
            for zeta in range(1, nz):
                g_z_in(zeta).wait_recv()
            g_x(x, 0, nz, 0, dev_a).start()
            g_x(x, 0, nz, 1, dev_b).start()
            g_d(x, core, 0).start()

        @pl.when(t == 5 + (s + 1) // 2)
        def _():
            g_x(na, 0, nz, 0, dev_a).wait_recv()
            g_x(nb, 0, nz, 1, dev_b).wait_recv()
            g_x(nb, 0, half, 2, dev_a).start()
            g_x(na, half, half, 3, dev_b).start()
            g_d(na, core, 1).start()
            g_d(nb, core, 2).start()

        @pl.when(t == 2 * (ns - 1) + mb - 1)
        def _():
            g_x(opp, 0, half, 2, dev_a).wait_recv()
            g_x(opp, half, half, 3, dev_b).wait_recv()
            g_d(opp, core, 3).start()

        @pl.when(jnp.logical_and(mf >= 0, mf < mb))
        def _():
            @pl.when(s > 0)
            def _():
                send_f(mf).wait_recv()

            xv = xin[mf].astype(F32)
            center = jnp.mean(xv, axis=-1, keepdims=True)
            dev = xv - center
            spread = jnp.mean(dev * dev, axis=-1, keepdims=True)
            scaled = lax.rsqrt(spread + 1e-05)
            normed = dev * scaled
            nf[mf] = normed
            scf[mf] = jnp.broadcast_to(scaled, (tok, 128))
            nbv = normed.astype(BF)
            left[0, mf] = nbv
            acc = xv
            for j in range(nt):
                cols = slice(j * tile, (j + 1) * tile)
                u = dot_nn(nbv, w[0, :, cols])
                uu = u * u
                bent = jnp.tanh(u * (gelu_coef + (gelu_coef * 0.044715) * uu))
                hu = 0.5 * u
                hp = 0.5 + 0.5 * bent
                hid = (u * hp).astype(BF)
                right[1, mf, :, cols] = hid
                slope[mf, :, cols] = hp + hu * (1.0 - bent * bent) * (
                    gelu_coef + (gelu_coef * 3.0 * 0.044715) * uu
                )
                acc = acc + dot_nt(hid, w[1, :, cols])

            @pl.when(s < ns - 1)
            def _():
                fout[mf] = acc.astype(BF)
                send_f(mf).start()

        @pl.when(jnp.logical_and(mbk >= 0, mbk < mb))
        def _():
            @pl.when(s < ns - 1)
            def _():
                send_b(mbk).wait_recv()

            g = left[1, mbk]
            for j in range(nt):
                cols = slice(j * tile, (j + 1) * tile)
                bh = dot_nn(g, w[1, :, cols])
                right[0, mbk, :, cols] = (bh * slope[mbk, :, cols]).astype(BF)

            @pl.when(s > 0)
            def _():
                bn = dot_nt(right[0, mbk], w[0])
                normed = nf[mbk]
                first = jnp.mean(bn, axis=-1, keepdims=True)
                second = jnp.mean(bn * normed, axis=-1, keepdims=True)
                sc = scf[mbk][:, :1]
                gout[mbk] = (g.astype(F32) + sc * (bn - first - normed * second)).astype(BF)
                send_b(mbk).start()

    cp_we.wait()
    cp_ow.wait()
    cp_var.wait()
    cp_se.wait()
    for k, xx in enumerate((x, na, nb, opp)):
        g_d(xx, 1 - core, k).wait_recv()

    qx = NX // 2
    ct = 512 if hc % 512 == 0 else 256
    nct = hc // ct
    rows = qx * nz * NC * 16

    def first_pass(idx, sq):
        i = idx // nct
        j = pl.multiple_of((idx % nct) * ct, ct)
        lt = left[i].reshape(mb * tok, d)
        rt = right[i, :, :, pl.ds(j, ct)].reshape(mb * tok, ct)
        grad = dot_tn(lt, rt)
        shared = mom[pl.ds(i * qx, qx), :, :, :, pl.ds(j, ct)].reshape(rows, ct).astype(F32)
        err = we[pl.ds(i * qx, qx), :, :, :, pl.ds(j, ct)].reshape(rows, ct).astype(F32)
        c = 0.9 * shared + 0.1 * grad + err
        comb[pl.ds(i * qx, qx), :, :, :, pl.ds(j, ct)] = c.reshape(qx, nz, NC, 16, ct)
        return sq + jnp.sum((c * c).reshape(rows // 8, 8, ct), axis=0)

    sq = lax.fori_loop(0, 2 * nct, first_pass, jnp.zeros((8, ct), F32))
    total_sq = jnp.sum(jnp.sum(sq, axis=0, keepdims=True), axis=1, keepdims=True)
    scale = jnp.sqrt(total_sq * (1.0 / (2 * d * hc)) + 0.01)
    inverse = 1.0 / scale

    def second_pass(q):
        @pl.loop(0, nz)
        def _(k):
            c = comb[q, k].reshape(NC * 16, hc)
            p = (scale * jnp.tanh(c * inverse)).astype(BF)
            packed[q, k] = p.reshape(NC, 16, hc)
            ne[q, k] = (c - p.astype(F32)).astype(BF).reshape(NC, 16, hc)

    def to_partner(q, k):
        return remote(packed.at[q, pl.ds(0, nz), 1 - core], d0.at[k], d_s.at[k], d_r.at[k], partner)

    def pair_sum(q, k):
        to_partner(q, k).wait_recv()

        @pl.loop(0, nz)
        def _(i):
            zeta = half + i // 2 - (i % 2) * (1 + 2 * (i // 2))
            zz = (z + zeta) % nz
            s0[k, i] = (packed[q, zz, core].astype(F32) + d0[k, zz].astype(F32)).astype(BF)

    def grp(ref, g):
        return ref.at[pl.ds(g * ng, ng)]

    def send_opp(g):
        to = dev_a if g % 2 == 0 else dev_b
        return remote(grp(s0.at[0], g), grp(ra, g), a_s.at[g], a_r.at[g], to)

    def send_a(g):
        return remote(grp(s0.at[1], g), grp(fa, g), ta_s.at[g], ta_r.at[g], dev_a)

    def send_bb(g):
        return remote(grp(s0.at[2], g), grp(fb, g), tb_s.at[g], tb_r.at[g], dev_b)

    def augment(g):
        send_opp(g).wait_recv()
        slot = 2 if g % 2 == 0 else 1

        @pl.loop(0, ng)
        def _(i):
            k = g * ng + i
            s0[slot, k] = (s0[slot, k].astype(F32) + ra[k].astype(F32)).astype(BF)

        (send_bb if slot == 2 else send_a)(g).start()

    def z_of(k):
        return half + k // 2 if k % 2 == 0 else half - 1 - k // 2

    def send_z(k):
        return remote(s1.at[k], zr.at[k], z_s.at[k], z_r.at[k], dev_z(z_of(k)))

    def along_z(groups):
        for g in groups:
            send_a(g).wait_recv()
            send_bb(g).wait_recv()
            for i in range(ng):
                k = g * ng + i
                s1[k] = (s0[3, k].astype(F32) + fa[k].astype(F32) + fb[k].astype(F32)).astype(BF)
                if z_of(k):
                    send_z(k).start()

    second_pass(opp)
    to_partner(opp, 0).start()
    second_pass(na)
    to_partner(na, 1).start()
    pair_sum(opp, 0)
    send_opp(0).start()
    send_opp(1).start()
    second_pass(nb)
    to_partner(nb, 2).start()
    pair_sum(na, 1)
    send_a(0).start()
    second_pass(x)
    to_partner(x, 3).start()
    pair_sum(nb, 2)
    send_bb(1).start()
    send_opp(2).start()
    send_opp(3).start()
    augment(0)
    augment(1)
    send_a(2).start()
    send_bb(3).start()
    pair_sum(x, 3)
    augment(2)
    augment(3)
    along_z((0, 1))
    along_z((2, 3))

    total = s1[nz - 1].astype(F32)
    for k in range(nz - 1):
        send_z(k).wait_recv()
        total = total + zr[k].astype(F32)
    merged = total * (1.0 / (NX * nz * NC)) + se[0]
    msq = jnp.sum(jnp.sum(merged * merged, axis=0, keepdims=True), axis=1, keepdims=True)
    sscale = jnp.sqrt(msq * (1.0 / (16 * hc)) + 0.01)
    values = (sscale * jnp.tanh(merged * (1.0 / sscale))).astype(BF)
    vf = values.astype(F32)
    nm_ref[0] = values
    nse_ref[0] = merged - vf
    step = 0.01 * vf / (jnp.sqrt(var[0].astype(F32)) + 1e-08)
    nw_ref[0] = (own_w[...].astype(F32) - step).astype(BF)

    for m in range(mb):
        @pl.when(s < ns - 1)
        def _():
            send_f(m).wait_send()

        @pl.when(s > 0)
        def _():
            send_b(m).wait_send()

    for zeta in range(1, nz):
        g_z(zeta).wait_send()
    g_x(x, 0, nz, 0, dev_a).wait_send()
    g_x(x, 0, nz, 1, dev_b).wait_send()
    g_x(nb, 0, half, 2, dev_a).wait_send()
    g_x(na, half, half, 3, dev_b).wait_send()
    for k, xx in enumerate((x, na, nb, opp)):
        g_d(xx, core, k).wait_send()
    for k, q in enumerate((opp, na, nb, x)):
        to_partner(q, k).wait_send()
    for g in range(4):
        send_opp(g).wait_send()
        send_a(g).wait_send()
        send_bb(g).wait_send()
    for k in range(nz - 1):
        send_z(k).wait_send()


def store_kernel(a, b, c, e, a_out, b_out, c_out, e_out, sems):
    copies = [
        pltpu.make_async_copy(src, dst, sems.at[k])
        for k, (src, dst) in enumerate(((c, c_out), (e, e_out), (a, a_out), (b, b_out)))
    ]
    for copy in copies:
        copy.start()
    for copy in copies:
        copy.wait()


def local(ns, nz, token_ids, embed, weights, variance, momentum, worker_error, server_error, cotangent):
    mb, tok = token_ids.shape
    d = embed.shape[1]
    hc = weights.shape[3]
    dims = (NX, nz, NC, 16, hc)
    vm = pl.BlockSpec(memory_space=pltpu.VMEM)
    hbm = pl.BlockSpec(memory_space=pl.ANY)
    dma = pltpu.SemaphoreType.DMA
    tile = 512 if hc % 512 == 0 else 128
    kernel = functools.partial(step_kernel, ns, nz, mb, tok, d, hc, tile)
    nw, nm, ne, nse = pl.pallas_call(
        kernel,
        out_shape=(
            pltpu.VMEM((1, 16, hc), BF),
            pltpu.VMEM((1, 16, hc), BF),
            pltpu.VMEM(dims, BF),
            pltpu.VMEM((1, 16, hc), F32),
        ),
        in_specs=[hbm] * 8,
        out_specs=(vm, vm, vm, vm),
        scratch_shapes=[
            pltpu.VMEM((mb, tok), jnp.int32),
            pltpu.VMEM(embed.shape, BF),
            pltpu.VMEM((1, 16, hc), BF),
            pltpu.VMEM((1, 16, hc), F32),
            pltpu.VMEM((2, d, hc), BF),
            pltpu.VMEM((16, hc), BF),
            pltpu.VMEM(dims, BF),
            pltpu.VMEM(dims, BF),
            pltpu.VMEM(dims, F32),
            pltpu.VMEM(dims, BF),
            pltpu.VMEM((mb, tok, d), BF),
            pltpu.VMEM((mb, tok, d), BF),
            pltpu.VMEM((mb, tok, d), BF),
            pltpu.VMEM((mb, tok, d), F32),
            pltpu.VMEM((mb, tok, 128), F32),
            pltpu.VMEM((mb, tok, hc), F32),
            pltpu.VMEM((2, mb, tok, d), BF),
            pltpu.VMEM((2, mb, tok, hc), BF),
            pltpu.VMEM((4, nz, 16, hc), BF),
            pltpu.VMEM((4, nz, 16, hc), BF),
            pltpu.VMEM((nz, 16, hc), BF),
            pltpu.VMEM((nz, 16, hc), BF),
            pltpu.VMEM((nz, 16, hc), BF),
            pltpu.VMEM((nz, 16, hc), BF),
            pltpu.VMEM((nz, 16, hc), BF),
            dma((10,)),
            dma((mb,)), dma((mb,)), dma((mb,)), dma((mb,)),
            dma((nz - 1,)), dma((nz - 1,)), dma((4,)), dma((4,)), dma((4,)), dma((4,)),
            dma((4,)), dma((4,)), dma((4,)), dma((4,)), dma((4,)), dma((4,)), dma((4,)), dma((4,)),
            dma((nz,)), dma((nz,)),
        ],
        compiler_params=pltpu.CompilerParams(
            collective_id=0, has_side_effects=True, vmem_limit_bytes=48 * 1024 * 1024
        ),
        name="step",
    )(*(
        pltpu.with_memory_space_constraint(a, pltpu.MemorySpace.HBM)
        for a in (
            token_ids, embed, weights, variance, momentum,
            worker_error.reshape(dims), server_error, cotangent,
        )
    ))
    arrays = (nw, nm, ne, nse)
    nw, nm, ne, nse = pl.pallas_call(
        store_kernel,
        out_shape=tuple(jax.ShapeDtypeStruct(a.shape, a.dtype) for a in arrays),
        in_specs=[vm] * 4,
        out_specs=(hbm,) * 4,
        scratch_shapes=[dma((4,))],
        compiler_params=pltpu.CompilerParams(vmem_limit_bytes=4 * 1024 * 1024),
        name="store",
    )(*(pltpu.with_memory_space_constraint(a, pltpu.MemorySpace.VMEM) for a in arrays))
    return (nw, nm, ne.reshape(worker_error.shape), nse)


def solution(mesh):
    ns = mesh.shape["section"]
    nz = mesh.shape["dp"] // (NX * NC)
    in_specs = (
        P(None, "dp"),
        P(),
        P("section", None, None, None),
        P("section", "dp", None),
        P("section", "dp", None),
        P("section", "dp", None, None, None),
        P("section", "dp", None),
        P(None, "dp", None),
    )
    out_specs = (
        P("section", "dp", None),
        P("section", "dp", None),
        P("section", "dp", None, None, None),
        P("section", "dp", None),
    )
    return jax.shard_map(
        functools.partial(local, ns, nz), mesh=mesh, in_specs=in_specs, out_specs=out_specs,
        check_vma=False,
    )
```

```python
import functools
import math

import jax
import jax.numpy as jnp
from jax import lax
from jax.experimental import pallas as pl
from jax.experimental.pallas import tpu as pltpu
from jax.sharding import PartitionSpec as P

gelu_coef = math.sqrt(2.0 / math.pi)
MESH = pl.DeviceIdType.MESH
BF = jnp.bfloat16
F32 = jnp.float32
NX = 4
NC = 2


def dot_nn(a, b):
    return lax.dot_general(a, b, (((1,), (0,)), ((), ())), preferred_element_type=F32)


def dot_nt(a, b):
    return lax.dot_general(a, b, (((1,), (1,)), ((), ())), preferred_element_type=F32)


def dot_tn(a, b):
    return lax.dot_general(a, b, (((0,), (0,)), ((), ())), preferred_element_type=F32)


def step_kernel(
    ns, nz, mb, tok, d, hc, tile,
    ids_hbm, embed_hbm, w_hbm, var_hbm, mom_hbm, we_hbm, se_hbm, cot_hbm,
    nw_ref, nm_ref, ne, nse_ref,
    ids, embed, var, se, w, wt, own_w, we, mom, comb, packed, xin, fout, gout, nf, scf, slope, left, right,
    d0, s0, ra, fa, fb, s1, zr,
    loc, f_s, f_r, b_s, b_r, gz_s, gz_r, gx_s, gx_r, gy_s, gy_r, gd_s, gd_r,
    d_s, d_r, a_s, a_r, ta_s, ta_r, tb_s, tb_r, z_s, z_r,
):
    s = lax.axis_index("section")
    r = lax.axis_index("dp")
    core = r % NC
    z = (r // NC) % nz
    x = r // (NC * nz)
    na = x + 1 - 2 * (x % 2)
    nb = 3 - x
    opp = (x + 2) % 4
    half = nz // 2

    def at(xx, zz, cc):
        return (xx * nz + zz) * NC + cc

    partner = at(x, z, 1 - core)
    dev_a = at(na, z, core)
    dev_b = at(nb, z, core)

    def dev_z(zeta):
        return at(x, (z + zeta) % nz, core)

    def remote(src, dst, send, recv, to):
        return pltpu.make_async_remote_copy(
            src_ref=src, dst_ref=dst, send_sem=send, recv_sem=recv,
            device_id={"dp": to}, device_id_type=MESH,
        )

    barrier = pltpu.get_barrier_semaphore()
    for peer in [partner, dev_a, dev_b] + [dev_z(k) for k in range(1, nz)]:
        pl.semaphore_signal(barrier, inc=1, device_id={"dp": peer}, device_id_type=MESH)

    @pl.when(s > 0)
    def _():
        pl.semaphore_signal(barrier, inc=1, device_id={"section": s - 1}, device_id_type=MESH)

    @pl.when(s < ns - 1)
    def _():
        pl.semaphore_signal(barrier, inc=1, device_id={"section": s + 1}, device_id_type=MESH)

    cp_mom = pltpu.make_async_copy(mom_hbm.at[0], mom.at[x, z, core], loc.at[0])
    cp_w0 = pltpu.make_async_copy(w_hbm.at[0, 0], w.at[0], loc.at[1])
    cp_w1 = pltpu.make_async_copy(w_hbm.at[0, 1], w.at[1], loc.at[2])
    cp_we = pltpu.make_async_copy(we_hbm, we, loc.at[3])
    cp_ow = pltpu.make_async_copy(
        w_hbm.at[0, x // 2, pl.ds(pl.multiple_of((r % (NC * nz * 2)) * 16, 16), 16)], own_w, loc.at[4]
    )
    cp_ids = pltpu.make_async_copy(ids_hbm, ids, loc.at[5])
    cp_embed = pltpu.make_async_copy(embed_hbm, embed, loc.at[6])
    cp_var = pltpu.make_async_copy(var_hbm, var, loc.at[7])
    cp_se = pltpu.make_async_copy(se_hbm, se, loc.at[8])
    cp_cot = pltpu.make_async_copy(cot_hbm, left.at[1], loc.at[9])
    @pl.when(s == 0)
    def _():
        cp_ids.start()
        cp_embed.start()

    cp_w1.start()
    cp_w0.start()
    cp_mom.start()

    @pl.when(s == ns - 1)
    def _():
        cp_cot.start()

    cp_ow.start()
    cp_var.start()
    cp_se.start()

    @pl.when(s == 0)
    def _():
        vocab = embed.shape[0]
        cp_ids.wait()
        cp_embed.wait()
        for m in range(mb):
            hot = (
                lax.broadcasted_iota(jnp.int32, (vocab, tok), 0) == ids[m : m + 1, :]
            ).astype(F32).astype(BF)
            xin[m] = dot_tn(hot, embed[...]).astype(BF)

    def transposed(i):
        step = 256 if hc % 256 == 0 else hc

        @pl.loop(0, hc // step)
        def _(j):
            lo = pl.multiple_of(j * step, step)
            wt[i, pl.ds(lo, step), :] = w[i, :, pl.ds(lo, step)].T

    @pl.when(s == ns - 1)
    def _():
        cp_cot.wait()

    cp_w1.wait()
    transposed(1)
    cp_w0.wait()

    pl.semaphore_wait(
        barrier, 2 + nz + jnp.where(s > 0, 1, 0) + jnp.where(s < ns - 1, 1, 0)
    )

    cp_mom.wait()
    order = [0]
    for dist in range(1, half):
        order += [dist, nz - dist]
    order.append(half)
    parts = (range(0, half + 1), range(half + 1, nz))

    def mom_at(xx, k):
        return mom.at[xx, (z + order[k]) % nz, core]

    def g_z(k):
        blk = mom.at[x, z, core]
        return remote(blk, blk, gz_s.at[k], gz_r.at[order.index((nz - order[k]) % nz)], dev_z(order[k]))

    def g_z_in(k):
        blk = mom_at(x, k)
        return remote(blk, blk, gz_s.at[k], gz_r.at[k], dev_z(order[k]))

    def g_x(xx, k, j):
        blk = mom_at(xx, k)
        return remote(blk, blk, gx_s.at[j, k], gx_r.at[j, k], (dev_a, dev_b)[j])

    def g_y(xx, k):
        blk = mom_at(xx, k)
        return remote(blk, blk, gy_s.at[k], gy_r.at[k], (dev_a, dev_b)[k % 2])

    def g_d(j, xx, k, cc):
        blk = mom.at[xx, (z + order[k]) % nz, cc]
        return remote(blk, blk, gd_s.at[j, k], gd_r.at[j, k], partner)

    for k in range(1, nz):
        g_z(k).start()

    cp_we.start()

    def from_z(part):
        for k in parts[part]:
            if k:
                g_z_in(k).wait_recv()
            g_x(x, k, 0).start()
            g_x(x, k, 1).start()
            g_d(0, x, k, core).start()

    def from_x(part):
        for k in parts[part]:
            g_x(na, k, 0).wait_recv()
            g_x(nb, k, 1).wait_recv()
            g_y(nb if k % 2 == 0 else na, k).start()
            g_d(1, na, k, core).start()
            g_d(2, nb, k, core).start()

    def from_far():
        for k in range(nz):
            g_y(opp, k).wait_recv()
            g_d(3, opp, k, core).start()

    def send_f(m):
        return pltpu.make_async_remote_copy(
            src_ref=fout.at[m], dst_ref=xin.at[m], send_sem=f_s.at[m], recv_sem=f_r.at[m],
            device_id={"section": jnp.minimum(s + 1, ns - 1)}, device_id_type=MESH,
        )

    def send_b(m):
        return pltpu.make_async_remote_copy(
            src_ref=gout.at[m], dst_ref=left.at[1, m], send_sem=b_s.at[m], recv_sem=b_r.at[m],
            device_id={"section": jnp.maximum(s - 1, 0)}, device_id_type=MESH,
        )

    nt = hc // tile

    slots = 2 * (ns - 1) + mb
    first_b = jnp.where(s == ns - 1, ns - 1, jnp.maximum(2 * (ns - 1) - s, s + mb - 1))

    def slot_of(*by_section):
        at_t = jnp.int32(min(by_section[-1], slots - 1))
        for sec, value in enumerate(by_section[:-1]):
            at_t = jnp.where(s == sec, min(value, slots - 1), at_t)
        return at_t

    t_near = slot_of(4, 5, 0, 0)
    t_next = slot_of(4, 5, 6, 5)
    t_last = slot_of(4, 6, 8, 7)
    t_far = slot_of(7, 8, 9, 8)

    @pl.loop(0, slots)
    def _(t):
        mf = t - s
        mbk = t - first_b

        @pl.when(jnp.logical_and(t == 0, s > 0))
        def _():
            transposed(0)

        @pl.when(t == t_near)
        def _():
            from_z(0)

        @pl.when(t == t_next)
        def _():
            from_z(1)
            from_x(0)

        @pl.when(t == t_last)
        def _():
            from_x(1)

        @pl.when(t == t_far)
        def _():
            from_far()

        @pl.when(jnp.logical_and(mf >= 0, mf < mb))
        def _():
            @pl.when(s > 0)
            def _():
                send_f(mf).wait_recv()

            xv = xin[mf].astype(F32)
            center = jnp.mean(xv, axis=-1, keepdims=True)
            dev = xv - center
            spread = jnp.mean(dev * dev, axis=-1, keepdims=True)
            scaled = lax.rsqrt(spread + 1e-05)
            normed = dev * scaled
            nf[mf] = normed
            scf[mf] = jnp.broadcast_to(scaled, (tok, 128))
            nbv = normed.astype(BF)
            left[0, mf] = nbv
            acc = xv
            for j in range(nt):
                cols = slice(j * tile, (j + 1) * tile)
                u = dot_nn(nbv, w[0, :, cols])
                uu = u * u
                bent = jnp.tanh(u * (gelu_coef + (gelu_coef * 0.044715) * uu))
                hu = 0.5 * u
                hp = 0.5 + 0.5 * bent
                hid = (u * hp).astype(BF)
                right[1, mf, :, cols] = hid
                slope[mf, :, cols] = hp + hu * (1.0 - bent * bent) * (
                    gelu_coef + (gelu_coef * 3.0 * 0.044715) * uu
                )
                acc = acc + dot_nn(hid, wt[1, cols, :])

            @pl.when(s < ns - 1)
            def _():
                fout[mf] = acc.astype(BF)
                send_f(mf).start()

        @pl.when(jnp.logical_and(mbk >= 0, mbk < mb))
        def _():
            @pl.when(s < ns - 1)
            def _():
                send_b(mbk).wait_recv()

            g = left[1, mbk]
            for j in range(nt):
                cols = slice(j * tile, (j + 1) * tile)
                bh = dot_nn(g, w[1, :, cols])
                right[0, mbk, :, cols] = (bh * slope[mbk, :, cols]).astype(BF)

            @pl.when(s > 0)
            def _():
                bn = dot_nn(right[0, mbk], wt[0])
                normed = nf[mbk]
                first = jnp.mean(bn, axis=-1, keepdims=True)
                second = jnp.mean(bn * normed, axis=-1, keepdims=True)
                sc = scf[mbk][:, :1]
                gout[mbk] = (g.astype(F32) + sc * (bn - first - normed * second)).astype(BF)
                send_b(mbk).start()

    cp_we.wait()
    cp_ow.wait()
    cp_var.wait()
    cp_se.wait()
    for j, xx in enumerate((x, na, nb, opp)):
        for k in range(nz):
            g_d(j, xx, k, 1 - core).wait_recv()

    qx = NX // 2
    ct = 512 if hc % 512 == 0 else 256
    nct = hc // ct
    rows = qx * nz * NC * 16

    def first_pass(idx, sq):
        i = idx // nct
        j = pl.multiple_of((idx % nct) * ct, ct)
        lt = left[i].reshape(mb * tok, d)
        rt = right[i, :, :, pl.ds(j, ct)].reshape(mb * tok, ct)
        grad = dot_tn(lt, rt)
        shared = mom[pl.ds(i * qx, qx), :, :, :, pl.ds(j, ct)].reshape(rows, ct).astype(F32)
        err = we[pl.ds(i * qx, qx), :, :, :, pl.ds(j, ct)].reshape(rows, ct).astype(F32)
        c = 0.9 * shared + 0.1 * grad + err
        comb[pl.ds(i * qx, qx), :, :, :, pl.ds(j, ct)] = c.reshape(qx, nz, NC, 16, ct)
        return sq + jnp.sum((c * c).reshape(rows // 8, 8, ct), axis=0)

    sq = lax.fori_loop(0, 2 * nct, first_pass, jnp.zeros((8, ct), F32))
    total_sq = jnp.sum(jnp.sum(sq, axis=0, keepdims=True), axis=1, keepdims=True)
    scale = jnp.sqrt(total_sq * (1.0 / (2 * d * hc)) + 0.01)
    inverse = 1.0 / scale

    def second_pass(q):
        @pl.loop(0, nz)
        def _(k):
            c = comb[q, k].reshape(NC * 16, hc)
            p = (scale * jnp.tanh(c * inverse)).astype(BF)
            packed[q, k] = p.reshape(NC, 16, hc)
            ne[q, k] = (c - p.astype(F32)).astype(BF).reshape(NC, 16, hc)

    def to_partner(q, k):
        return remote(packed.at[q, pl.ds(0, nz), 1 - core], d0.at[k], d_s.at[k], d_r.at[k], partner)

    def pair_sum(q, k):
        to_partner(q, k).wait_recv()

        @pl.loop(0, nz)
        def _(i):
            zeta = half + (i % 2) * ((i + 1) // 2 + i // 2) - i // 2
            zz = (z + zeta) % nz
            s0[k, i] = (packed[q, zz, core].astype(F32) + d0[k, zz].astype(F32)).astype(BF)

    def send_opp(g):
        to = dev_a if g % 2 == 0 else dev_b
        return remote(s0.at[0, g], ra.at[g], a_s.at[g], a_r.at[g], to)

    def send_a(g):
        return remote(s0.at[1, g], fa.at[g], ta_s.at[g], ta_r.at[g], dev_a)

    def send_bb(g):
        return remote(s0.at[2, g], fb.at[g], tb_s.at[g], tb_r.at[g], dev_b)

    def far(p):
        send_opp(2 * p).start()
        send_opp(2 * p + 1).start()

    def near(p):
        send_a(2 * p).start()
        send_bb(2 * p + 1).start()

    def augment(p):
        for g in (2 * p, 2 * p + 1):
            send_opp(g).wait_recv()
            slot = 2 if g % 2 == 0 else 1
            s0[slot, g] = (s0[slot, g].astype(F32) + ra[g].astype(F32)).astype(BF)
            (send_bb if slot == 2 else send_a)(g).start()

    def z_of(k):
        return (half + (k + 1) // 2 if k % 2 else half - k // 2) % nz

    def send_z(k):
        return remote(s1.at[k], zr.at[k], z_s.at[k], z_r.at[k], dev_z(z_of(k)))

    def along_z(p):
        for k in (2 * p, 2 * p + 1):
            send_a(k).wait_recv()
            send_bb(k).wait_recv()
            s1[k] = (s0[3, k].astype(F32) + fa[k].astype(F32) + fb[k].astype(F32)).astype(BF)
            if z_of(k):
                send_z(k).start()

    rounds = nz // 2
    second_pass(opp)
    to_partner(opp, 0).start()
    second_pass(na)
    to_partner(na, 1).start()
    pair_sum(opp, 0)
    far(0)
    second_pass(nb)
    to_partner(nb, 2).start()
    pair_sum(na, 1)
    second_pass(x)
    to_partner(x, 3).start()
    pair_sum(nb, 2)
    near(0)
    far(1)
    augment(0)
    near(1)
    if rounds > 2:
        far(2)
    pair_sum(x, 3)
    augment(1)
    if rounds > 2:
        near(2)
        far(3)
        along_z(0)
        augment(2)
        near(3)
        along_z(1)
        augment(3)
        along_z(2)
        along_z(3)
    else:
        along_z(0)
        along_z(1)

    total = s1[nz - 1].astype(F32)
    for k in range(nz - 1):
        send_z(k).wait_recv()
        total = total + zr[k].astype(F32)
    merged = total * (1.0 / (NX * nz * NC)) + se[0]
    msq = jnp.sum(jnp.sum(merged * merged, axis=0, keepdims=True), axis=1, keepdims=True)
    sscale = jnp.sqrt(msq * (1.0 / (16 * hc)) + 0.01)
    values = (sscale * jnp.tanh(merged * (1.0 / sscale))).astype(BF)
    vf = values.astype(F32)
    nm_ref[0] = values
    nse_ref[0] = merged - vf
    step = 0.01 * vf / (jnp.sqrt(var[0].astype(F32)) + 1e-08)
    nw_ref[0] = (own_w[...].astype(F32) - step).astype(BF)

    for m in range(mb):
        @pl.when(s < ns - 1)
        def _():
            send_f(m).wait_send()

        @pl.when(s > 0)
        def _():
            send_b(m).wait_send()

    for k in range(1, nz):
        g_z(k).wait_send()
    for k in range(nz):
        g_x(x, k, 0).wait_send()
        g_x(x, k, 1).wait_send()
        g_y(nb if k % 2 == 0 else na, k).wait_send()
        for j, xx in enumerate((x, na, nb, opp)):
            g_d(j, xx, k, core).wait_send()
    for k, q in enumerate((opp, na, nb, x)):
        to_partner(q, k).wait_send()
    for g in range(nz):
        send_opp(g).wait_send()
        send_a(g).wait_send()
        send_bb(g).wait_send()
    for k in range(nz - 1):
        send_z(k).wait_send()


def store_kernel(a, b, c, e, a_out, b_out, c_out, e_out, sems):
    copies = [
        pltpu.make_async_copy(src, dst, sems.at[k])
        for k, (src, dst) in enumerate(((c, c_out), (e, e_out), (a, a_out), (b, b_out)))
    ]
    for copy in copies:
        copy.start()
    for copy in copies:
        copy.wait()


def local(ns, nz, token_ids, embed, weights, variance, momentum, worker_error, server_error, cotangent):
    mb, tok = token_ids.shape
    d = embed.shape[1]
    hc = weights.shape[3]
    dims = (NX, nz, NC, 16, hc)
    vm = pl.BlockSpec(memory_space=pltpu.VMEM)
    hbm = pl.BlockSpec(memory_space=pl.ANY)
    dma = pltpu.SemaphoreType.DMA
    tile = 512 if hc % 512 == 0 else 128
    kernel = functools.partial(step_kernel, ns, nz, mb, tok, d, hc, tile)
    nw, nm, ne, nse = pl.pallas_call(
        kernel,
        out_shape=(
            pltpu.VMEM((1, 16, hc), BF),
            pltpu.VMEM((1, 16, hc), BF),
            pltpu.VMEM(dims, BF),
            pltpu.VMEM((1, 16, hc), F32),
        ),
        in_specs=[hbm] * 8,
        out_specs=(vm, vm, vm, vm),
        scratch_shapes=[
            pltpu.VMEM((mb, tok), jnp.int32),
            pltpu.VMEM(embed.shape, BF),
            pltpu.VMEM((1, 16, hc), BF),
            pltpu.VMEM((1, 16, hc), F32),
            pltpu.VMEM((2, d, hc), BF),
            pltpu.VMEM((2, hc, d), BF),
            pltpu.VMEM((16, hc), BF),
            pltpu.VMEM(dims, BF),
            pltpu.VMEM(dims, BF),
            pltpu.VMEM(dims, F32),
            pltpu.VMEM(dims, BF),
            pltpu.VMEM((mb, tok, d), BF),
            pltpu.VMEM((mb, tok, d), BF),
            pltpu.VMEM((mb, tok, d), BF),
            pltpu.VMEM((mb, tok, d), F32),
            pltpu.VMEM((mb, tok, 128), F32),
            pltpu.VMEM((mb, tok, hc), F32),
            pltpu.VMEM((2, mb, tok, d), BF),
            pltpu.VMEM((2, mb, tok, hc), BF),
            pltpu.VMEM((4, nz, 16, hc), BF),
            pltpu.VMEM((4, nz, 16, hc), BF),
            pltpu.VMEM((nz, 16, hc), BF),
            pltpu.VMEM((nz, 16, hc), BF),
            pltpu.VMEM((nz, 16, hc), BF),
            pltpu.VMEM((nz, 16, hc), BF),
            pltpu.VMEM((nz, 16, hc), BF),
            dma((10,)),
            dma((mb,)), dma((mb,)), dma((mb,)), dma((mb,)),
            dma((nz,)), dma((nz,)), dma((2, nz)), dma((2, nz)), dma((nz,)), dma((nz,)), dma((4, nz)), dma((4, nz)),
            dma((4,)), dma((4,)), dma((nz,)), dma((nz,)), dma((nz,)), dma((nz,)), dma((nz,)), dma((nz,)),
            dma((nz,)), dma((nz,)),
        ],
        compiler_params=pltpu.CompilerParams(
            collective_id=0, has_side_effects=True, vmem_limit_bytes=48 * 1024 * 1024
        ),
        name="step",
    )(*(
        pltpu.with_memory_space_constraint(a, pltpu.MemorySpace.HBM)
        for a in (
            token_ids, embed, weights, variance, momentum,
            worker_error.reshape(dims), server_error, cotangent,
        )
    ))
    arrays = (nw, nm, ne, nse)
    nw, nm, ne, nse = pl.pallas_call(
        store_kernel,
        out_shape=tuple(jax.ShapeDtypeStruct(a.shape, a.dtype) for a in arrays),
        in_specs=[vm] * 4,
        out_specs=(hbm,) * 4,
        scratch_shapes=[dma((4,))],
        compiler_params=pltpu.CompilerParams(vmem_limit_bytes=4 * 1024 * 1024),
        name="store",
    )(*(pltpu.with_memory_space_constraint(a, pltpu.MemorySpace.VMEM) for a in arrays))
    return (nw, nm, ne.reshape(worker_error.shape), nse)


def solution(mesh):
    ns = mesh.shape["section"]
    nz = mesh.shape["dp"] // (NX * NC)
    in_specs = (
        P(None, "dp"),
        P(),
        P("section", None, None, None),
        P("section", "dp", None),
        P("section", "dp", None),
        P("section", "dp", None, None, None),
        P("section", "dp", None),
        P(None, "dp", None),
    )
    out_specs = (
        P("section", "dp", None),
        P("section", "dp", None),
        P("section", "dp", None, None, None),
        P("section", "dp", None),
    )
    return jax.shard_map(
        functools.partial(local, ns, nz), mesh=mesh, in_specs=in_specs, out_specs=out_specs,
        check_vma=False,
    )
```

```python
import functools
import math

import jax
import jax.numpy as jnp
from jax import lax
from jax.experimental import pallas as pl
from jax.experimental.pallas import tpu as pltpu
from jax.sharding import PartitionSpec as P

gelu_coef = math.sqrt(2.0 / math.pi)
MESH = pl.DeviceIdType.MESH
BF = jnp.bfloat16
F32 = jnp.float32
NX = 4
NC = 2


def dot_nn(a, b):
    return lax.dot_general(a, b, (((1,), (0,)), ((), ())), preferred_element_type=F32)


def dot_nt(a, b):
    return lax.dot_general(a, b, (((1,), (1,)), ((), ())), preferred_element_type=F32)


def dot_tn(a, b):
    return lax.dot_general(a, b, (((0,), (0,)), ((), ())), preferred_element_type=F32)


def step_kernel(
    ns, nz, mb, tok, d, hc, tile,
    ids_hbm, embed_hbm, w_hbm, var_hbm, mom_hbm, we_hbm, se_hbm, cot_hbm,
    nw_ref, nm_ref, ne, nse_ref,
    ids, embed, var, se, w, wt, own_w, we, mom, comb, packed, xin, fout, gout, nf, scf, slope, left, right,
    d0, s0, ra, fa, fb, s1, zr,
    loc, f_s, f_r, b_s, b_r, gz_s, gz_r, gx_s, gx_r, gy_s, gy_r, gd_s, gd_r,
    d_s, d_r, a_s, a_r, ta_s, ta_r, tb_s, tb_r, z_s, z_r,
):
    s = lax.axis_index("section")
    r = lax.axis_index("dp")
    core = r % NC
    z = (r // NC) % nz
    x = r // (NC * nz)
    na = x + 1 - 2 * (x % 2)
    nb = 3 - x
    opp = (x + 2) % 4
    half = nz // 2

    def at(xx, zz, cc):
        return (xx * nz + zz) * NC + cc

    partner = at(x, z, 1 - core)
    dev_a = at(na, z, core)
    dev_b = at(nb, z, core)

    def dev_z(zeta):
        return at(x, (z + zeta) % nz, core)

    def remote(src, dst, send, recv, to):
        return pltpu.make_async_remote_copy(
            src_ref=src, dst_ref=dst, send_sem=send, recv_sem=recv,
            device_id={"dp": to}, device_id_type=MESH,
        )

    barrier = pltpu.get_barrier_semaphore()
    for peer in [partner, dev_a, dev_b] + [dev_z(k) for k in range(1, nz)]:
        pl.semaphore_signal(barrier, inc=1, device_id={"dp": peer}, device_id_type=MESH)

    @pl.when(s > 0)
    def _():
        pl.semaphore_signal(barrier, inc=1, device_id={"section": s - 1}, device_id_type=MESH)

    @pl.when(s < ns - 1)
    def _():
        pl.semaphore_signal(barrier, inc=1, device_id={"section": s + 1}, device_id_type=MESH)

    cp_mom = pltpu.make_async_copy(mom_hbm.at[0], mom.at[x, z, core], loc.at[0])
    cp_w0 = pltpu.make_async_copy(w_hbm.at[0, 0], w.at[0], loc.at[1])
    cp_w1 = pltpu.make_async_copy(w_hbm.at[0, 1], w.at[1], loc.at[2])
    cp_we = pltpu.make_async_copy(we_hbm, we, loc.at[3])
    cp_ow = pltpu.make_async_copy(
        w_hbm.at[0, x // 2, pl.ds(pl.multiple_of((r % (NC * nz * 2)) * 16, 16), 16)], own_w, loc.at[4]
    )
    cp_ids = pltpu.make_async_copy(ids_hbm, ids, loc.at[5])
    cp_embed = pltpu.make_async_copy(embed_hbm, embed, loc.at[6])
    cp_var = pltpu.make_async_copy(var_hbm, var, loc.at[7])
    cp_se = pltpu.make_async_copy(se_hbm, se, loc.at[8])
    cp_cot = pltpu.make_async_copy(cot_hbm, left.at[1], loc.at[9])
    @pl.when(s == 0)
    def _():
        cp_ids.start()
        cp_embed.start()

    cp_w0.start()
    cp_w1.start()
    cp_mom.start()

    @pl.when(s == ns - 1)
    def _():
        cp_cot.start()

    cp_ow.start()
    cp_var.start()
    cp_se.start()

    @pl.when(s == 0)
    def _():
        vocab = embed.shape[0]
        cp_ids.wait()
        cp_embed.wait()
        for m in range(mb):
            hot = (
                lax.broadcasted_iota(jnp.int32, (vocab, tok), 0) == ids[m : m + 1, :]
            ).astype(F32).astype(BF)
            xin[m] = dot_tn(hot, embed[...]).astype(BF)

    def transposed(i):
        step = 256 if hc % 256 == 0 else hc

        @pl.loop(0, hc // step)
        def _(j):
            lo = pl.multiple_of(j * step, step)
            wt[i, pl.ds(lo, step), :] = w[i, :, pl.ds(lo, step)].T

    @pl.when(s == ns - 1)
    def _():
        cp_cot.wait()

    cp_w0.wait()
    cp_w1.wait()

    order = [0]
    for dist in range(1, half):
        order += [dist, nz - dist]
    order.append(half)
    parts = (range(0, half + 1), range(half + 1, nz))

    def mom_at(xx, k):
        return mom.at[xx, (z + order[k]) % nz, core]

    def g_z(k):
        blk = mom.at[x, z, core]
        return remote(blk, blk, gz_s.at[k], gz_r.at[order.index((nz - order[k]) % nz)], dev_z(order[k]))

    def g_z_in(k):
        blk = mom_at(x, k)
        return remote(blk, blk, gz_s.at[k], gz_r.at[k], dev_z(order[k]))

    def g_x(xx, k, j):
        blk = mom_at(xx, k)
        return remote(blk, blk, gx_s.at[j, k], gx_r.at[j, k], (dev_a, dev_b)[j])

    def g_y(xx, k):
        blk = mom_at(xx, k)
        return remote(blk, blk, gy_s.at[k], gy_r.at[k], (dev_a, dev_b)[k % 2])

    def g_d(j, xx, k, cc):
        blk = mom.at[xx, (z + order[k]) % nz, cc]
        return remote(blk, blk, gd_s.at[j, k], gd_r.at[j, k], partner)

    def from_z(part):
        for k in parts[part]:
            if k:
                g_z_in(k).wait_recv()
            g_x(x, k, 0).start()
            g_x(x, k, 1).start()
            g_d(0, x, k, core).start()

    def from_x(part):
        for k in parts[part]:
            g_x(na, k, 0).wait_recv()
            g_x(nb, k, 1).wait_recv()
            g_y(nb if k % 2 == 0 else na, k).start()
            g_d(1, na, k, core).start()
            g_d(2, nb, k, core).start()

    def from_far():
        for k in range(nz):
            g_y(opp, k).wait_recv()
            g_d(3, opp, k, core).start()

    def add_shared(q, j):
        for k in range(nz):
            g_d(j, q, k, 1 - core).wait_recv()

        @pl.loop(0, nz)
        def _(k):
            comb[q, k] = 0.9 * mom[q, k].astype(F32) + we[q, k].astype(F32)

    def send_f(m):
        return pltpu.make_async_remote_copy(
            src_ref=fout.at[m], dst_ref=xin.at[m], send_sem=f_s.at[m], recv_sem=f_r.at[m],
            device_id={"section": jnp.minimum(s + 1, ns - 1)}, device_id_type=MESH,
        )

    def send_b(m):
        return pltpu.make_async_remote_copy(
            src_ref=gout.at[m], dst_ref=left.at[1, m], send_sem=b_s.at[m], recv_sem=b_r.at[m],
            device_id={"section": jnp.maximum(s - 1, 0)}, device_id_type=MESH,
        )

    nt = hc // tile

    def forward(m, second):
        xv = xin[m].astype(F32)
        center = jnp.mean(xv, axis=-1, keepdims=True)
        dev = xv - center
        spread = jnp.mean(dev * dev, axis=-1, keepdims=True)
        scaled = lax.rsqrt(spread + 1e-05)
        normed = dev * scaled
        nf[m] = normed
        scf[m] = jnp.broadcast_to(scaled, (tok, 128))
        nbv = normed.astype(BF)
        left[0, m] = nbv
        acc = xv
        for j in range(nt):
            cols = slice(j * tile, (j + 1) * tile)
            u = dot_nn(nbv, w[0, :, cols])
            uu = u * u
            bent = jnp.tanh(u * (gelu_coef + (gelu_coef * 0.044715) * uu))
            hu = 0.5 * u
            hp = 0.5 + 0.5 * bent
            hid = (u * hp).astype(BF)
            right[1, m, :, cols] = hid
            slope[m, :, cols] = hp + hu * (1.0 - bent * bent) * (
                gelu_coef + (gelu_coef * 3.0 * 0.044715) * uu
            )
            if second is not None:
                acc = acc + second(hid, cols)
        if second is not None:
            fout[m] = acc.astype(BF)

    slots = 2 * (ns - 1) + mb
    first_b = jnp.where(s == ns - 1, ns - 1, jnp.maximum(2 * (ns - 1) - s, s + mb - 1))

    def slot_of(*by_section):
        at_t = jnp.int32(min(by_section[-1], slots - 1))
        for sec, value in enumerate(by_section[:-1]):
            at_t = jnp.where(s == sec, min(value, slots - 1), at_t)
        return at_t

    t_near = slot_of(4, 5, 0, 0)
    t_next = slot_of(4, 5, 6, 5)
    t_last = slot_of(4, 6, 8, 7)
    t_far = slot_of(7, 8, 9, 8)
    t_shared = slot_of(5, 9, 9, 9)

    @pl.when(s == 0)
    def _():
        forward(0, lambda hid, cols: dot_nt(hid, w[1, :, cols]))

    pl.semaphore_wait(
        barrier, 2 + nz + jnp.where(s > 0, 1, 0) + jnp.where(s < ns - 1, 1, 0)
    )

    @pl.when(s == 0)
    def _():
        send_f(0).start()

    cp_mom.wait()
    for k in range(1, nz):
        g_z(k).start()
    cp_we.start()

    @pl.when(s > 0)
    def _():
        transposed(1)
        transposed(0)

    @pl.loop(0, slots)
    def _(t):
        mf = t - s
        mbk = t - first_b

        @pl.when(t == t_near)
        def _():
            from_z(0)

        @pl.when(t == t_next)
        def _():
            from_z(1)
            from_x(0)

        @pl.when(t == t_last)
        def _():
            from_x(1)

        @pl.when(t == t_far)
        def _():
            from_far()

        @pl.when(t == t_shared)
        def _():
            cp_we.wait()
            for j, q in enumerate((x, na, nb)):
                add_shared(q, j)

        @pl.when(t == slots - 1)
        def _():
            add_shared(opp, 3)

        has_f = jnp.logical_and(mf >= 0, mf < mb)

        @pl.when(jnp.logical_and(jnp.logical_and(has_f, s == 0), t > 0))
        def _():
            forward(mf, lambda hid, cols: dot_nt(hid, w[1, :, cols]))

        @pl.when(jnp.logical_and(has_f, jnp.logical_and(s > 0, s < ns - 1)))
        def _():
            send_f(mf).wait_recv()
            forward(mf, lambda hid, cols: dot_nn(hid, wt[1, cols, :]))

        @pl.when(jnp.logical_and(jnp.logical_and(has_f, s < ns - 1), t > 0))
        def _():
            send_f(mf).start()

        @pl.when(jnp.logical_and(has_f, s == ns - 1))
        def _():
            send_f(mf).wait_recv()
            forward(mf, None)

        @pl.when(jnp.logical_and(mbk >= 0, mbk < mb))
        def _():
            @pl.when(s < ns - 1)
            def _():
                send_b(mbk).wait_recv()

            g = left[1, mbk]
            for j in range(nt):
                cols = slice(j * tile, (j + 1) * tile)
                bh = dot_nn(g, w[1, :, cols])
                right[0, mbk, :, cols] = (bh * slope[mbk, :, cols]).astype(BF)

            @pl.when(s > 0)
            def _():
                bn = dot_nn(right[0, mbk], wt[0])
                normed = nf[mbk]
                first = jnp.mean(bn, axis=-1, keepdims=True)
                second = jnp.mean(bn * normed, axis=-1, keepdims=True)
                sc = scf[mbk][:, :1]
                gout[mbk] = (g.astype(F32) + sc * (bn - first - normed * second)).astype(BF)
                send_b(mbk).start()

    cp_ow.wait()
    cp_var.wait()
    cp_se.wait()

    qx = NX // 2
    ct = 512 if hc % 512 == 0 else 256
    nct = hc // ct
    rows = qx * nz * NC * 16

    def first_pass(idx, sq):
        i = idx // nct
        j = pl.multiple_of((idx % nct) * ct, ct)
        lt = left[i].reshape(mb * tok, d)
        rt = right[i, :, :, pl.ds(j, ct)].reshape(mb * tok, ct)
        grad = dot_tn(lt, rt)
        c = comb[pl.ds(i * qx, qx), :, :, :, pl.ds(j, ct)].reshape(rows, ct) + 0.1 * grad
        comb[pl.ds(i * qx, qx), :, :, :, pl.ds(j, ct)] = c.reshape(qx, nz, NC, 16, ct)
        return sq + jnp.sum((c * c).reshape(rows // 8, 8, ct), axis=0)

    sq = lax.fori_loop(0, 2 * nct, first_pass, jnp.zeros((8, ct), F32))
    total_sq = jnp.sum(jnp.sum(sq, axis=0, keepdims=True), axis=1, keepdims=True)
    scale = jnp.sqrt(total_sq * (1.0 / (2 * d * hc)) + 0.01)
    inverse = 1.0 / scale

    def second_pass(q):
        @pl.loop(0, nz)
        def _(k):
            c = comb[q, k].reshape(NC * 16, hc)
            p = (scale * jnp.tanh(c * inverse)).astype(BF)
            packed[q, k] = p.reshape(NC, 16, hc)
            ne[q, k] = (c - p.astype(F32)).astype(BF).reshape(NC, 16, hc)

    def to_partner(q, k):
        return remote(packed.at[q, pl.ds(0, nz), 1 - core], d0.at[k], d_s.at[k], d_r.at[k], partner)

    def pair_sum(q, k):
        to_partner(q, k).wait_recv()

        @pl.loop(0, nz)
        def _(i):
            zeta = half + (i % 2) * ((i + 1) // 2 + i // 2) - i // 2
            zz = (z + zeta) % nz
            s0[k, i] = (packed[q, zz, core].astype(F32) + d0[k, zz].astype(F32)).astype(BF)

    def send_opp(g):
        to = dev_a if g % 2 == 0 else dev_b
        return remote(s0.at[0, g], ra.at[g], a_s.at[g], a_r.at[g], to)

    def send_a(g):
        return remote(s0.at[1, g], fa.at[g], ta_s.at[g], ta_r.at[g], dev_a)

    def send_bb(g):
        return remote(s0.at[2, g], fb.at[g], tb_s.at[g], tb_r.at[g], dev_b)

    def far(p):
        send_opp(2 * p).start()
        send_opp(2 * p + 1).start()

    def near(p):
        send_a(2 * p).start()
        send_bb(2 * p + 1).start()

    def augment(p):
        for g in (2 * p, 2 * p + 1):
            send_opp(g).wait_recv()
            slot = 2 if g % 2 == 0 else 1
            s0[slot, g] = (s0[slot, g].astype(F32) + ra[g].astype(F32)).astype(BF)
            (send_bb if slot == 2 else send_a)(g).start()

    def z_of(k):
        return (half + (k + 1) // 2 if k % 2 else half - k // 2) % nz

    def send_z(k):
        return remote(s1.at[k], zr.at[k], z_s.at[k], z_r.at[k], dev_z(z_of(k) if k else nz - 1))

    def along_z(p):
        for k in (2 * p, 2 * p + 1):
            send_a(k).wait_recv()
            send_bb(k).wait_recv()
            s1[k] = (s0[3, k].astype(F32) + fa[k].astype(F32) + fb[k].astype(F32)).astype(BF)
            if z_of(k) and k != 1:
                send_z(k).start()

    def relayed():
        send_z(0).wait_recv()
        s1[1] = (s1[1].astype(F32) + zr[0].astype(F32)).astype(BF)
        send_z(1).start()

    rounds = nz // 2
    second_pass(opp)
    to_partner(opp, 0).start()
    second_pass(na)
    to_partner(na, 1).start()
    pair_sum(opp, 0)
    far(0)
    second_pass(nb)
    to_partner(nb, 2).start()
    pair_sum(na, 1)
    second_pass(x)
    to_partner(x, 3).start()
    pair_sum(nb, 2)
    near(0)
    far(1)
    augment(0)
    near(1)
    if rounds > 2:
        far(2)
    pair_sum(x, 3)
    augment(1)
    if rounds > 2:
        near(2)
        far(3)
        along_z(0)
        augment(2)
        near(3)
        along_z(1)
        relayed()
        augment(3)
        along_z(2)
        along_z(3)
    else:
        along_z(0)
        relayed()
        along_z(1)

    total = s1[nz - 1].astype(F32)
    for k in range(1, nz - 1):
        send_z(k).wait_recv()
        total = total + zr[k].astype(F32)
    merged = total * (1.0 / (NX * nz * NC)) + se[0]
    msq = jnp.sum(jnp.sum(merged * merged, axis=0, keepdims=True), axis=1, keepdims=True)
    sscale = jnp.sqrt(msq * (1.0 / (16 * hc)) + 0.01)
    values = (sscale * jnp.tanh(merged * (1.0 / sscale))).astype(BF)
    vf = values.astype(F32)
    nm_ref[0] = values
    nse_ref[0] = merged - vf
    step = 0.01 * vf / (jnp.sqrt(var[0].astype(F32)) + 1e-08)
    nw_ref[0] = (own_w[...].astype(F32) - step).astype(BF)

    for m in range(mb):
        @pl.when(s < ns - 1)
        def _():
            send_f(m).wait_send()

        @pl.when(s > 0)
        def _():
            send_b(m).wait_send()

    for k in range(1, nz):
        g_z(k).wait_send()
    for k in range(nz):
        g_x(x, k, 0).wait_send()
        g_x(x, k, 1).wait_send()
        g_y(nb if k % 2 == 0 else na, k).wait_send()
        for j, xx in enumerate((x, na, nb, opp)):
            g_d(j, xx, k, core).wait_send()
    for k, q in enumerate((opp, na, nb, x)):
        to_partner(q, k).wait_send()
    for g in range(nz):
        send_opp(g).wait_send()
        send_a(g).wait_send()
        send_bb(g).wait_send()
    for k in range(nz - 1):
        send_z(k).wait_send()


def store_kernel(a, b, c, e, a_out, b_out, c_out, e_out, sems):
    copies = [
        pltpu.make_async_copy(src, dst, sems.at[k])
        for k, (src, dst) in enumerate(((c, c_out), (e, e_out), (a, a_out), (b, b_out)))
    ]
    for copy in copies:
        copy.start()
    for copy in copies:
        copy.wait()


def local(ns, nz, token_ids, embed, weights, variance, momentum, worker_error, server_error, cotangent):
    mb, tok = token_ids.shape
    d = embed.shape[1]
    hc = weights.shape[3]
    dims = (NX, nz, NC, 16, hc)
    vm = pl.BlockSpec(memory_space=pltpu.VMEM)
    hbm = pl.BlockSpec(memory_space=pl.ANY)
    dma = pltpu.SemaphoreType.DMA
    tile = 512 if hc % 512 == 0 else 128
    kernel = functools.partial(step_kernel, ns, nz, mb, tok, d, hc, tile)
    nw, nm, ne, nse = pl.pallas_call(
        kernel,
        out_shape=(
            pltpu.VMEM((1, 16, hc), BF),
            pltpu.VMEM((1, 16, hc), BF),
            pltpu.VMEM(dims, BF),
            pltpu.VMEM((1, 16, hc), F32),
        ),
        in_specs=[hbm] * 8,
        out_specs=(vm, vm, vm, vm),
        scratch_shapes=[
            pltpu.VMEM((mb, tok), jnp.int32),
            pltpu.VMEM(embed.shape, BF),
            pltpu.VMEM((1, 16, hc), BF),
            pltpu.VMEM((1, 16, hc), F32),
            pltpu.VMEM((2, d, hc), BF),
            pltpu.VMEM((2, hc, d), BF),
            pltpu.VMEM((16, hc), BF),
            pltpu.VMEM(dims, BF),
            pltpu.VMEM(dims, BF),
            pltpu.VMEM(dims, F32),
            pltpu.VMEM(dims, BF),
            pltpu.VMEM((mb, tok, d), BF),
            pltpu.VMEM((mb, tok, d), BF),
            pltpu.VMEM((mb, tok, d), BF),
            pltpu.VMEM((mb, tok, d), F32),
            pltpu.VMEM((mb, tok, 128), F32),
            pltpu.VMEM((mb, tok, hc), F32),
            pltpu.VMEM((2, mb, tok, d), BF),
            pltpu.VMEM((2, mb, tok, hc), BF),
            pltpu.VMEM((4, nz, 16, hc), BF),
            pltpu.VMEM((4, nz, 16, hc), BF),
            pltpu.VMEM((nz, 16, hc), BF),
            pltpu.VMEM((nz, 16, hc), BF),
            pltpu.VMEM((nz, 16, hc), BF),
            pltpu.VMEM((nz, 16, hc), BF),
            pltpu.VMEM((nz, 16, hc), BF),
            dma((10,)),
            dma((mb,)), dma((mb,)), dma((mb,)), dma((mb,)),
            dma((nz,)), dma((nz,)), dma((2, nz)), dma((2, nz)), dma((nz,)), dma((nz,)), dma((4, nz)), dma((4, nz)),
            dma((4,)), dma((4,)), dma((nz,)), dma((nz,)), dma((nz,)), dma((nz,)), dma((nz,)), dma((nz,)),
            dma((nz,)), dma((nz,)),
        ],
        compiler_params=pltpu.CompilerParams(
            collective_id=0, has_side_effects=True, vmem_limit_bytes=48 * 1024 * 1024
        ),
        name="step",
    )(*(
        pltpu.with_memory_space_constraint(a, pltpu.MemorySpace.HBM)
        for a in (
            token_ids, embed, weights, variance, momentum,
            worker_error.reshape(dims), server_error, cotangent,
        )
    ))
    arrays = (nw, nm, ne, nse)
    nw, nm, ne, nse = pl.pallas_call(
        store_kernel,
        out_shape=tuple(jax.ShapeDtypeStruct(a.shape, a.dtype) for a in arrays),
        in_specs=[vm] * 4,
        out_specs=(hbm,) * 4,
        scratch_shapes=[dma((4,))],
        compiler_params=pltpu.CompilerParams(vmem_limit_bytes=4 * 1024 * 1024),
        name="store",
    )(*(pltpu.with_memory_space_constraint(a, pltpu.MemorySpace.VMEM) for a in arrays))
    return (nw, nm, ne.reshape(worker_error.shape), nse)


def solution(mesh):
    ns = mesh.shape["section"]
    nz = mesh.shape["dp"] // (NX * NC)
    in_specs = (
        P(None, "dp"),
        P(),
        P("section", None, None, None),
        P("section", "dp", None),
        P("section", "dp", None),
        P("section", "dp", None, None, None),
        P("section", "dp", None),
        P(None, "dp", None),
    )
    out_specs = (
        P("section", "dp", None),
        P("section", "dp", None),
        P("section", "dp", None, None, None),
        P("section", "dp", None),
    )
    return jax.shard_map(
        functools.partial(local, ns, nz), mesh=mesh, in_specs=in_specs, out_specs=out_specs,
        check_vma=False,
    )
```

```python
import functools
import math

import jax
import jax.numpy as jnp
from jax import lax
from jax.experimental import pallas as pl
from jax.experimental.pallas import tpu as pltpu
from jax.sharding import PartitionSpec as P

gelu_coef = math.sqrt(2.0 / math.pi)
MESH = pl.DeviceIdType.MESH
BF = jnp.bfloat16
F32 = jnp.float32
NX = 4
NC = 2


def dot_nn(a, b):
    return lax.dot_general(a, b, (((1,), (0,)), ((), ())), preferred_element_type=F32)


def dot_nt(a, b):
    return lax.dot_general(a, b, (((1,), (1,)), ((), ())), preferred_element_type=F32)


def dot_tn(a, b):
    return lax.dot_general(a, b, (((0,), (0,)), ((), ())), preferred_element_type=F32)


def step_kernel(
    ns, nz, mb, tok, d, hc, tile,
    ids_hbm, embed_hbm, w_hbm, var_hbm, mom_hbm, we_hbm, se_hbm, cot_hbm,
    nw_ref, nm_ref, ne, nse_ref,
    ids, embed, var, se, w, wt, own_w, we, mom, comb, packed, xin, fout, gout, nf, scf, slope, left, right, lt,
    d0, s0, ra, fa, fb, s1, zr,
    loc, f_s, f_r, b_s, b_r, gz_s, gz_r, gx_s, gx_r, gy_s, gy_r, gd_s, gd_r,
    d_s, d_r, a_s, a_r, ta_s, ta_r, tb_s, tb_r, z_s, z_r,
):
    s = lax.axis_index("section")
    r = lax.axis_index("dp")
    core = r % NC
    z = (r // NC) % nz
    x = r // (NC * nz)
    na = x + 1 - 2 * (x % 2)
    nb = 3 - x
    opp = (x + 2) % 4
    half = nz // 2

    def at(xx, zz, cc):
        return (xx * nz + zz) * NC + cc

    partner = at(x, z, 1 - core)
    dev_a = at(na, z, core)
    dev_b = at(nb, z, core)

    def dev_z(zeta):
        return at(x, (z + zeta) % nz, core)

    def remote(src, dst, send, recv, to):
        return pltpu.make_async_remote_copy(
            src_ref=src, dst_ref=dst, send_sem=send, recv_sem=recv,
            device_id={"dp": to}, device_id_type=MESH,
        )

    barrier = pltpu.get_barrier_semaphore()
    for peer in [partner, dev_a, dev_b] + [dev_z(k) for k in range(1, nz)]:
        pl.semaphore_signal(barrier, inc=1, device_id={"dp": peer}, device_id_type=MESH)

    @pl.when(s > 0)
    def _():
        pl.semaphore_signal(barrier, inc=1, device_id={"section": s - 1}, device_id_type=MESH)

    @pl.when(s < ns - 1)
    def _():
        pl.semaphore_signal(barrier, inc=1, device_id={"section": s + 1}, device_id_type=MESH)

    cp_mom = pltpu.make_async_copy(mom_hbm.at[0], mom.at[x, z, core], loc.at[0])
    cp_w0 = pltpu.make_async_copy(w_hbm.at[0, 0], w.at[0], loc.at[1])
    cp_w1 = pltpu.make_async_copy(w_hbm.at[0, 1], w.at[1], loc.at[2])
    cp_we = pltpu.make_async_copy(we_hbm, we, loc.at[3])
    cp_ow = pltpu.make_async_copy(
        w_hbm.at[0, x // 2, pl.ds(pl.multiple_of((r % (NC * nz * 2)) * 16, 16), 16)], own_w, loc.at[4]
    )
    cp_ids = pltpu.make_async_copy(ids_hbm, ids, loc.at[5])
    cp_embed = pltpu.make_async_copy(embed_hbm, embed, loc.at[6])
    cp_var = pltpu.make_async_copy(var_hbm, var, loc.at[7])
    cp_se = pltpu.make_async_copy(se_hbm, se, loc.at[8])
    cp_cot = pltpu.make_async_copy(cot_hbm, left.at[1], loc.at[9])
    @pl.when(s == 0)
    def _():
        cp_ids.start()
        cp_embed.start()

    cp_w0.start()
    cp_w1.start()
    cp_mom.start()

    @pl.when(s == ns - 1)
    def _():
        cp_cot.start()

    cp_ow.start()
    cp_var.start()
    cp_se.start()

    @pl.when(s == 0)
    def _():
        vocab = embed.shape[0]
        cp_ids.wait()
        cp_embed.wait()
        for m in range(mb):
            hot = (
                lax.broadcasted_iota(jnp.int32, (vocab, tok), 0) == ids[m : m + 1, :]
            ).astype(F32).astype(BF)
            xin[m] = dot_tn(hot, embed[...]).astype(BF)

    def transposed(i):
        step = 256 if hc % 256 == 0 else hc

        @pl.loop(0, hc // step)
        def _(j):
            lo = pl.multiple_of(j * step, step)
            wt[i, pl.ds(lo, step), :] = w[i, :, pl.ds(lo, step)].T

    @pl.when(s == ns - 1)
    def _():
        cp_cot.wait()

    cp_w0.wait()
    cp_w1.wait()

    order = [0]
    for dist in range(1, half):
        order += [dist, nz - dist]
    order.append(half)
    parts = (range(0, half + 1), range(half + 1, nz))

    def mom_at(xx, k):
        return mom.at[xx, (z + order[k]) % nz, core]

    def g_z(k):
        blk = mom.at[x, z, core]
        return remote(blk, blk, gz_s.at[k], gz_r.at[order.index((nz - order[k]) % nz)], dev_z(order[k]))

    def g_z_in(k):
        blk = mom_at(x, k)
        return remote(blk, blk, gz_s.at[k], gz_r.at[k], dev_z(order[k]))

    def g_x(xx, k, j):
        blk = mom_at(xx, k)
        return remote(blk, blk, gx_s.at[j, k], gx_r.at[j, k], (dev_a, dev_b)[j])

    def g_y(xx, k):
        blk = mom_at(xx, k)
        return remote(blk, blk, gy_s.at[k], gy_r.at[k], (dev_a, dev_b)[k % 2])

    def g_d(j, xx, k, cc):
        blk = mom.at[xx, (z + order[k]) % nz, cc]
        return remote(blk, blk, gd_s.at[j, k], gd_r.at[j, k], partner)

    def from_z(part):
        for k in parts[part]:
            if k:
                g_z_in(k).wait_recv()
            g_x(x, k, 0).start()
            g_x(x, k, 1).start()
            g_d(0, x, k, core).start()

    def from_x(part):
        for k in parts[part]:
            g_x(na, k, 0).wait_recv()
            g_x(nb, k, 1).wait_recv()
            g_y(nb if k % 2 == 0 else na, k).start()
            g_d(1, na, k, core).start()
            g_d(2, nb, k, core).start()

    def from_far():
        for k in range(nz):
            g_y(opp, k).wait_recv()
            g_d(3, opp, k, core).start()

    def add_shared(q, j):
        for k in range(nz):
            g_d(j, q, k, 1 - core).wait_recv()

        @pl.loop(0, nz)
        def _(k):
            comb[q, k] = 0.9 * mom[q, k].astype(F32) + we[q, k].astype(F32)

    def flip(i):
        lt[i] = left[i].reshape(mb * tok, d).T

    def send_f(m):
        return pltpu.make_async_remote_copy(
            src_ref=fout.at[m], dst_ref=xin.at[m], send_sem=f_s.at[m], recv_sem=f_r.at[m],
            device_id={"section": jnp.minimum(s + 1, ns - 1)}, device_id_type=MESH,
        )

    def send_b(m):
        return pltpu.make_async_remote_copy(
            src_ref=gout.at[m], dst_ref=left.at[1, m], send_sem=b_s.at[m], recv_sem=b_r.at[m],
            device_id={"section": jnp.maximum(s - 1, 0)}, device_id_type=MESH,
        )

    nt = hc // tile

    def forward(m, second):
        xv = xin[m].astype(F32)
        center = jnp.mean(xv, axis=-1, keepdims=True)
        dev = xv - center
        spread = jnp.mean(dev * dev, axis=-1, keepdims=True)
        scaled = lax.rsqrt(spread + 1e-05)
        normed = dev * scaled
        nf[m] = normed
        scf[m] = jnp.broadcast_to(scaled, (tok, 128))
        nbv = normed.astype(BF)
        left[0, m] = nbv
        acc = xv
        for j in range(nt):
            cols = slice(j * tile, (j + 1) * tile)
            u = dot_nn(nbv, w[0, :, cols])
            uu = u * u
            bent = jnp.tanh(u * (gelu_coef + (gelu_coef * 0.044715) * uu))
            hu = 0.5 * u
            hp = 0.5 + 0.5 * bent
            hid = (u * hp).astype(BF)
            right[1, m, :, cols] = hid
            slope[m, :, cols] = hp + hu * (1.0 - bent * bent) * (
                gelu_coef + (gelu_coef * 3.0 * 0.044715) * uu
            )
            if second is not None:
                acc = acc + second(hid, cols)
        if second is not None:
            fout[m] = acc.astype(BF)

    slots = 2 * (ns - 1) + mb
    first_b = jnp.where(s == ns - 1, ns - 1, jnp.maximum(2 * (ns - 1) - s, s + mb - 1))

    def slot_of(*by_section):
        at_t = jnp.int32(min(by_section[-1], slots - 1))
        for sec, value in enumerate(by_section[:-1]):
            at_t = jnp.where(s == sec, min(value, slots - 1), at_t)
        return at_t

    t_near = slot_of(4, 5, 0, 0)
    t_next = slot_of(4, 5, 6, 5)
    t_last = slot_of(4, 6, 8, 7)
    t_far = slot_of(7, 8, 9, 8)
    t_shared = slot_of(5, 9, 9, 9)

    @pl.when(s == 0)
    def _():
        forward(0, lambda hid, cols: dot_nt(hid, w[1, :, cols]))

    pl.semaphore_wait(
        barrier, 2 + nz + jnp.where(s > 0, 1, 0) + jnp.where(s < ns - 1, 1, 0)
    )

    @pl.when(s == 0)
    def _():
        send_f(0).start()

    cp_mom.wait()
    for k in range(1, nz):
        g_z(k).start()
    cp_we.start()

    @pl.when(s > 0)
    def _():
        transposed(1)
        transposed(0)

    @pl.loop(0, slots)
    def _(t):
        mf = t - s
        mbk = t - first_b

        @pl.when(t == t_near)
        def _():
            from_z(0)

        @pl.when(t == t_next)
        def _():
            from_z(1)
            from_x(0)

        @pl.when(t == t_last)
        def _():
            from_x(1)

        @pl.when(t == t_far)
        def _():
            from_far()

        @pl.when(t == t_shared)
        def _():
            cp_we.wait()
            for j, q in enumerate((x, na, nb)):
                add_shared(q, j)
            flip(0)

        @pl.when(t == slots - 1)
        def _():
            add_shared(opp, 3)

        has_f = jnp.logical_and(mf >= 0, mf < mb)

        @pl.when(jnp.logical_and(jnp.logical_and(has_f, s == 0), t > 0))
        def _():
            forward(mf, lambda hid, cols: dot_nt(hid, w[1, :, cols]))

        @pl.when(jnp.logical_and(has_f, jnp.logical_and(s > 0, s < ns - 1)))
        def _():
            send_f(mf).wait_recv()
            forward(mf, lambda hid, cols: dot_nn(hid, wt[1, cols, :]))

        @pl.when(jnp.logical_and(jnp.logical_and(has_f, s < ns - 1), t > 0))
        def _():
            send_f(mf).start()

        @pl.when(jnp.logical_and(has_f, s == ns - 1))
        def _():
            send_f(mf).wait_recv()
            forward(mf, None)

        @pl.when(jnp.logical_and(mbk >= 0, mbk < mb))
        def _():
            @pl.when(s < ns - 1)
            def _():
                send_b(mbk).wait_recv()

            g = left[1, mbk]
            for j in range(nt):
                cols = slice(j * tile, (j + 1) * tile)
                bh = dot_nn(g, w[1, :, cols])
                right[0, mbk, :, cols] = (bh * slope[mbk, :, cols]).astype(BF)

            @pl.when(s > 0)
            def _():
                bn = dot_nn(right[0, mbk], wt[0])
                normed = nf[mbk]
                first = jnp.mean(bn, axis=-1, keepdims=True)
                second = jnp.mean(bn * normed, axis=-1, keepdims=True)
                sc = scf[mbk][:, :1]
                gout[mbk] = (g.astype(F32) + sc * (bn - first - normed * second)).astype(BF)
                send_b(mbk).start()

    cp_ow.wait()
    cp_var.wait()
    cp_se.wait()

    qx = NX // 2
    ct = 512 if hc % 512 == 0 else 256
    nct = hc // ct
    rows = qx * nz * NC * 16

    def first_pass(idx, sq):
        i = idx // nct
        j = pl.multiple_of((idx % nct) * ct, ct)
        rt = right[i, :, :, pl.ds(j, ct)].reshape(mb * tok, ct)
        grad = dot_nn(lt[i], rt)
        c = comb[pl.ds(i * qx, qx), :, :, :, pl.ds(j, ct)].reshape(rows, ct) + 0.1 * grad
        comb[pl.ds(i * qx, qx), :, :, :, pl.ds(j, ct)] = c.reshape(qx, nz, NC, 16, ct)
        return sq + jnp.sum((c * c).reshape(rows // 8, 8, ct), axis=0)

    flip(1)
    sq = lax.fori_loop(0, 2 * nct, first_pass, jnp.zeros((8, ct), F32))
    total_sq = jnp.sum(jnp.sum(sq, axis=0, keepdims=True), axis=1, keepdims=True)
    scale = jnp.sqrt(total_sq * (1.0 / (2 * d * hc)) + 0.01)
    inverse = 1.0 / scale

    quarters = (opp, na, nb, x)

    def slot_z(k):
        zeta = half + (k % 2) * ((k + 1) // 2 + k // 2) - k // 2
        return (z + zeta) % nz

    def to_partner(j, k):
        return remote(
            packed.at[quarters[j], slot_z(k), 1 - core], d0.at[j, k], d_s.at[j, k], d_r.at[j, k], partner
        )

    def second_pass(j, lo, hi):
        q = quarters[j]

        @pl.loop(lo, hi)
        def _(k):
            zz = slot_z(k)
            c = comb[q, zz].reshape(NC * 16, hc)
            p = (scale * jnp.tanh(c * inverse)).astype(BF)
            packed[q, zz] = p.reshape(NC, 16, hc)
            ne[q, zz] = (c - p.astype(F32)).astype(BF).reshape(NC, 16, hc)
            to_partner(j, k).start()

    def pair_sum(j, lo, hi):
        @pl.loop(lo, hi)
        def _(k):
            to_partner(j, k).wait_recv()
            s0[j, k] = (packed[quarters[j], slot_z(k), core].astype(F32) + d0[j, k].astype(F32)).astype(BF)

    def pack(p):
        for j in range(3):
            second_pass(j, 2 * p, 2 * p + 2)

    def sum_far(p):
        pair_sum(0, 2 * p, 2 * p + 2)
        far(p)

    def sum_near(p):
        pair_sum(1, 2 * p, 2 * p + 2)
        pair_sum(2, 2 * p, 2 * p + 2)

    def send_opp(g):
        to = dev_a if g % 2 == 0 else dev_b
        return remote(s0.at[0, g], ra.at[g], a_s.at[g], a_r.at[g], to)

    def send_a(g):
        return remote(s0.at[1, g], fa.at[g], ta_s.at[g], ta_r.at[g], dev_a)

    def send_bb(g):
        return remote(s0.at[2, g], fb.at[g], tb_s.at[g], tb_r.at[g], dev_b)

    def far(p):
        send_opp(2 * p).start()
        send_opp(2 * p + 1).start()

    def near(p):
        send_a(2 * p).start()
        send_bb(2 * p + 1).start()

    def augment(p):
        for g in (2 * p, 2 * p + 1):
            send_opp(g).wait_recv()
            slot = 2 if g % 2 == 0 else 1
            s0[slot, g] = (s0[slot, g].astype(F32) + ra[g].astype(F32)).astype(BF)
            (send_bb if slot == 2 else send_a)(g).start()

    def z_of(k):
        return (half + (k + 1) // 2 if k % 2 else half - k // 2) % nz

    def send_z(k):
        return remote(s1.at[k], zr.at[k], z_s.at[k], z_r.at[k], dev_z(z_of(k) if k else nz - 1))

    def along_z(p):
        for k in (2 * p, 2 * p + 1):
            send_a(k).wait_recv()
            send_bb(k).wait_recv()
            s1[k] = (s0[3, k].astype(F32) + fa[k].astype(F32) + fb[k].astype(F32)).astype(BF)
            if z_of(k) and k != 1:
                send_z(k).start()

    def relayed():
        send_z(0).wait_recv()
        s1[1] = (s1[1].astype(F32) + zr[0].astype(F32)).astype(BF)
        send_z(1).start()

    rounds = nz // 2
    pack(0)
    pack(1)
    sum_far(0)
    sum_near(0)
    near(0)
    sum_far(1)
    sum_near(1)
    for p in range(2, rounds):
        pack(p)
    second_pass(3, 0, nz)
    augment(0)
    near(1)
    if rounds > 2:
        sum_far(2)
        sum_near(2)
    pair_sum(3, 0, nz)
    augment(1)
    if rounds > 2:
        near(2)
        sum_far(3)
        sum_near(3)
        along_z(0)
        augment(2)
        near(3)
        along_z(1)
        relayed()
        augment(3)
        along_z(2)
        along_z(3)
    else:
        along_z(0)
        relayed()
        along_z(1)

    total = s1[nz - 1].astype(F32)
    for k in range(1, nz - 1):
        send_z(k).wait_recv()
        total = total + zr[k].astype(F32)
    merged = total * (1.0 / (NX * nz * NC)) + se[0]
    msq = jnp.sum(jnp.sum(merged * merged, axis=0, keepdims=True), axis=1, keepdims=True)
    sscale = jnp.sqrt(msq * (1.0 / (16 * hc)) + 0.01)
    values = (sscale * jnp.tanh(merged * (1.0 / sscale))).astype(BF)
    vf = values.astype(F32)
    nm_ref[0] = values
    nse_ref[0] = merged - vf
    step = 0.01 * vf / (jnp.sqrt(var[0].astype(F32)) + 1e-08)
    nw_ref[0] = (own_w[...].astype(F32) - step).astype(BF)

    for m in range(mb):
        @pl.when(s < ns - 1)
        def _():
            send_f(m).wait_send()

        @pl.when(s > 0)
        def _():
            send_b(m).wait_send()

    for k in range(1, nz):
        g_z(k).wait_send()
    for k in range(nz):
        g_x(x, k, 0).wait_send()
        g_x(x, k, 1).wait_send()
        g_y(nb if k % 2 == 0 else na, k).wait_send()
        for j, xx in enumerate((x, na, nb, opp)):
            g_d(j, xx, k, core).wait_send()
    for j in range(4):
        for k in range(nz):
            to_partner(j, k).wait_send()
    for g in range(nz):
        send_opp(g).wait_send()
        send_a(g).wait_send()
        send_bb(g).wait_send()
    for k in range(nz - 1):
        send_z(k).wait_send()


def store_kernel(a, b, c, e, a_out, b_out, c_out, e_out, sems):
    copies = [
        pltpu.make_async_copy(src, dst, sems.at[k])
        for k, (src, dst) in enumerate(((c, c_out), (e, e_out), (a, a_out), (b, b_out)))
    ]
    for copy in copies:
        copy.start()
    for copy in copies:
        copy.wait()


def local(ns, nz, token_ids, embed, weights, variance, momentum, worker_error, server_error, cotangent):
    mb, tok = token_ids.shape
    d = embed.shape[1]
    hc = weights.shape[3]
    dims = (NX, nz, NC, 16, hc)
    vm = pl.BlockSpec(memory_space=pltpu.VMEM)
    hbm = pl.BlockSpec(memory_space=pl.ANY)
    dma = pltpu.SemaphoreType.DMA
    tile = 1024 if hc % 512 == 0 else 128
    kernel = functools.partial(step_kernel, ns, nz, mb, tok, d, hc, tile)
    nw, nm, ne, nse = pl.pallas_call(
        kernel,
        out_shape=(
            pltpu.VMEM((1, 16, hc), BF),
            pltpu.VMEM((1, 16, hc), BF),
            pltpu.VMEM(dims, BF),
            pltpu.VMEM((1, 16, hc), F32),
        ),
        in_specs=[hbm] * 8,
        out_specs=(vm, vm, vm, vm),
        scratch_shapes=[
            pltpu.VMEM((mb, tok), jnp.int32),
            pltpu.VMEM(embed.shape, BF),
            pltpu.VMEM((1, 16, hc), BF),
            pltpu.VMEM((1, 16, hc), F32),
            pltpu.VMEM((2, d, hc), BF),
            pltpu.VMEM((2, hc, d), BF),
            pltpu.VMEM((16, hc), BF),
            pltpu.VMEM(dims, BF),
            pltpu.VMEM(dims, BF),
            pltpu.VMEM(dims, F32),
            pltpu.VMEM(dims, BF),
            pltpu.VMEM((mb, tok, d), BF),
            pltpu.VMEM((mb, tok, d), BF),
            pltpu.VMEM((mb, tok, d), BF),
            pltpu.VMEM((mb, tok, d), F32),
            pltpu.VMEM((mb, tok, 128), F32),
            pltpu.VMEM((mb, tok, hc), F32),
            pltpu.VMEM((2, mb, tok, d), BF),
            pltpu.VMEM((2, mb, tok, hc), BF),
            pltpu.VMEM((2, d, mb * tok), BF),
            pltpu.VMEM((4, nz, 16, hc), BF),
            pltpu.VMEM((4, nz, 16, hc), BF),
            pltpu.VMEM((nz, 16, hc), BF),
            pltpu.VMEM((nz, 16, hc), BF),
            pltpu.VMEM((nz, 16, hc), BF),
            pltpu.VMEM((nz, 16, hc), BF),
            pltpu.VMEM((nz, 16, hc), BF),
            dma((10,)),
            dma((mb,)), dma((mb,)), dma((mb,)), dma((mb,)),
            dma((nz,)), dma((nz,)), dma((2, nz)), dma((2, nz)), dma((nz,)), dma((nz,)), dma((4, nz)), dma((4, nz)),
            dma((4, nz)), dma((4, nz)), dma((nz,)), dma((nz,)), dma((nz,)), dma((nz,)), dma((nz,)), dma((nz,)),
            dma((nz,)), dma((nz,)),
        ],
        compiler_params=pltpu.CompilerParams(
            collective_id=0, has_side_effects=True, vmem_limit_bytes=48 * 1024 * 1024
        ),
        name="step",
    )(*(
        pltpu.with_memory_space_constraint(a, pltpu.MemorySpace.HBM)
        for a in (
            token_ids, embed, weights, variance, momentum,
            worker_error.reshape(dims), server_error, cotangent,
        )
    ))
    arrays = (nw, nm, ne, nse)
    nw, nm, ne, nse = pl.pallas_call(
        store_kernel,
        out_shape=tuple(jax.ShapeDtypeStruct(a.shape, a.dtype) for a in arrays),
        in_specs=[vm] * 4,
        out_specs=(hbm,) * 4,
        scratch_shapes=[dma((4,))],
        compiler_params=pltpu.CompilerParams(vmem_limit_bytes=4 * 1024 * 1024),
        name="store",
    )(*(pltpu.with_memory_space_constraint(a, pltpu.MemorySpace.VMEM) for a in arrays))
    return (nw, nm, ne.reshape(worker_error.shape), nse)


def solution(mesh):
    ns = mesh.shape["section"]
    nz = mesh.shape["dp"] // (NX * NC)
    in_specs = (
        P(None, "dp"),
        P(),
        P("section", None, None, None),
        P("section", "dp", None),
        P("section", "dp", None),
        P("section", "dp", None, None, None),
        P("section", "dp", None),
        P(None, "dp", None),
    )
    out_specs = (
        P("section", "dp", None),
        P("section", "dp", None),
        P("section", "dp", None, None, None),
        P("section", "dp", None),
    )
    return jax.shard_map(
        functools.partial(local, ns, nz), mesh=mesh, in_specs=in_specs, out_specs=out_specs,
        check_vma=False,
    )
```

```python
import functools
import math

import jax
import jax.numpy as jnp
from jax import lax
from jax.experimental import pallas as pl
from jax.experimental.pallas import tpu as pltpu
from jax.sharding import PartitionSpec as P

gelu_coef = math.sqrt(2.0 / math.pi)
MESH = pl.DeviceIdType.MESH
BF = jnp.bfloat16
F32 = jnp.float32
NX = 4
NC = 2


def dot_nn(a, b):
    return lax.dot_general(a, b, (((1,), (0,)), ((), ())), preferred_element_type=F32)


def dot_nt(a, b):
    return lax.dot_general(a, b, (((1,), (1,)), ((), ())), preferred_element_type=F32)


def dot_tn(a, b):
    return lax.dot_general(a, b, (((0,), (0,)), ((), ())), preferred_element_type=F32)


def step_kernel(
    ns, nz, mb, tok, d, hc, tile,
    ids_hbm, embed_hbm, w_hbm, var_hbm, mom_hbm, we_hbm, se_hbm, cot_hbm,
    nw_ref, nm_ref, ne, nse_ref,
    ids, embed, var, se, w, wt, own_w, we, mom, comb, packed, xin, fout, gout, nf, scf, slope, left, right, lt,
    d0, s0, ra, fa, fb, s1, zr,
    loc, f_s, f_r, b_s, b_r, gz_s, gz_r, gx_s, gx_r, gy_s, gy_r, gd_s, gd_r,
    d_s, d_r, a_s, a_r, ta_s, ta_r, tb_s, tb_r, z_s, z_r,
):
    s = lax.axis_index("section")
    r = lax.axis_index("dp")
    core = r % NC
    z = (r // NC) % nz
    x = r // (NC * nz)
    na = x + 1 - 2 * (x % 2)
    nb = 3 - x
    opp = (x + 2) % 4
    half = nz // 2

    def at(xx, zz, cc):
        return (xx * nz + zz) * NC + cc

    partner = at(x, z, 1 - core)
    dev_a = at(na, z, core)
    dev_b = at(nb, z, core)

    def dev_z(zeta):
        return at(x, (z + zeta) % nz, core)

    def remote(src, dst, send, recv, to):
        return pltpu.make_async_remote_copy(
            src_ref=src, dst_ref=dst, send_sem=send, recv_sem=recv,
            device_id={"dp": to}, device_id_type=MESH,
        )

    barrier = pltpu.get_barrier_semaphore()
    for peer in [partner, dev_a, dev_b] + [dev_z(k) for k in range(1, nz)]:
        pl.semaphore_signal(barrier, inc=1, device_id={"dp": peer}, device_id_type=MESH)

    @pl.when(s > 0)
    def _():
        pl.semaphore_signal(barrier, inc=1, device_id={"section": s - 1}, device_id_type=MESH)

    @pl.when(s < ns - 1)
    def _():
        pl.semaphore_signal(barrier, inc=1, device_id={"section": s + 1}, device_id_type=MESH)

    cp_mom = pltpu.make_async_copy(mom_hbm.at[0], mom.at[x, z, core], loc.at[0])
    cp_w0 = pltpu.make_async_copy(w_hbm.at[0, 0], w.at[0], loc.at[1])
    cp_w1 = pltpu.make_async_copy(w_hbm.at[0, 1], w.at[1], loc.at[2])
    cp_we = pltpu.make_async_copy(we_hbm, we, loc.at[3])
    cp_ow = pltpu.make_async_copy(
        w_hbm.at[0, x // 2, pl.ds(pl.multiple_of((r % (NC * nz * 2)) * 16, 16), 16)], own_w, loc.at[4]
    )
    cp_ids = pltpu.make_async_copy(ids_hbm, ids, loc.at[5])
    cp_embed = pltpu.make_async_copy(embed_hbm, embed, loc.at[6])
    cp_var = pltpu.make_async_copy(var_hbm, var, loc.at[7])
    cp_se = pltpu.make_async_copy(se_hbm, se, loc.at[8])
    cp_cot = pltpu.make_async_copy(cot_hbm, left.at[1], loc.at[9])
    @pl.when(s == 0)
    def _():
        cp_ids.start()
        cp_embed.start()

    cp_w0.start()
    cp_w1.start()
    cp_mom.start()

    @pl.when(s == ns - 1)
    def _():
        cp_cot.start()

    cp_ow.start()
    cp_var.start()
    cp_se.start()

    @pl.when(s == 0)
    def _():
        vocab = embed.shape[0]
        cp_ids.wait()
        cp_embed.wait()
        for m in range(mb):
            hot = (
                lax.broadcasted_iota(jnp.int32, (vocab, tok), 0) == ids[m : m + 1, :]
            ).astype(F32).astype(BF)
            xin[m] = dot_tn(hot, embed[...]).astype(BF)

    def transposed(i):
        step = 256 if hc % 256 == 0 else hc

        @pl.loop(0, hc // step)
        def _(j):
            lo = pl.multiple_of(j * step, step)
            wt[i, pl.ds(lo, step), :] = w[i, :, pl.ds(lo, step)].T

    @pl.when(s == ns - 1)
    def _():
        cp_cot.wait()

    cp_w0.wait()
    cp_w1.wait()

    order = [0]
    for dist in range(1, half):
        order += [dist, nz - dist]
    order.append(half)
    parts = (range(0, half + 1), range(half + 1, nz))

    def mom_at(xx, k):
        return mom.at[xx, (z + order[k]) % nz, core]

    def g_z(k):
        blk = mom.at[x, z, core]
        return remote(blk, blk, gz_s.at[k], gz_r.at[order.index((nz - order[k]) % nz)], dev_z(order[k]))

    def g_z_in(k):
        blk = mom_at(x, k)
        return remote(blk, blk, gz_s.at[k], gz_r.at[k], dev_z(order[k]))

    def g_x(xx, k, j):
        blk = mom_at(xx, k)
        return remote(blk, blk, gx_s.at[j, k], gx_r.at[j, k], (dev_a, dev_b)[j])

    def g_y(xx, k):
        blk = mom_at(xx, k)
        return remote(blk, blk, gy_s.at[k], gy_r.at[k], (dev_a, dev_b)[k % 2])

    def g_d(j, xx, k, cc):
        blk = mom.at[xx, (z + order[k]) % nz, cc]
        return remote(blk, blk, gd_s.at[j, k], gd_r.at[j, k], partner)

    def from_z(part):
        for k in parts[part]:
            if k:
                g_z_in(k).wait_recv()
            g_x(x, k, 0).start()
            g_x(x, k, 1).start()
            g_d(0, x, k, core).start()

    def from_x(part):
        for k in parts[part]:
            g_x(na, k, 0).wait_recv()
            g_x(nb, k, 1).wait_recv()
            g_y(nb if k % 2 == 0 else na, k).start()
            g_d(1, na, k, core).start()
            g_d(2, nb, k, core).start()

    def from_far():
        for k in range(nz):
            g_y(opp, k).wait_recv()
            g_d(3, opp, k, core).start()

    def add_shared(q, j):
        for k in range(nz):
            g_d(j, q, k, 1 - core).wait_recv()

        @pl.loop(0, nz)
        def _(k):
            comb[q, k] = 0.9 * mom[q, k].astype(F32) + we[q, k].astype(F32)

    def flip(i):
        lt[i] = left[i].reshape(mb * tok, d).T

    def send_f(m):
        return pltpu.make_async_remote_copy(
            src_ref=fout.at[m], dst_ref=xin.at[m], send_sem=f_s.at[m], recv_sem=f_r.at[m],
            device_id={"section": jnp.minimum(s + 1, ns - 1)}, device_id_type=MESH,
        )

    def send_b(m):
        return pltpu.make_async_remote_copy(
            src_ref=gout.at[m], dst_ref=left.at[1, m], send_sem=b_s.at[m], recv_sem=b_r.at[m],
            device_id={"section": jnp.maximum(s - 1, 0)}, device_id_type=MESH,
        )

    nt = hc // tile

    def forward(m, second):
        xv = xin[m].astype(F32)
        center = jnp.mean(xv, axis=-1, keepdims=True)
        dev = xv - center
        spread = jnp.mean(dev * dev, axis=-1, keepdims=True)
        scaled = lax.rsqrt(spread + 1e-05)
        normed = dev * scaled
        nf[m] = normed
        scf[m] = jnp.broadcast_to(scaled, (tok, 128))
        nbv = normed.astype(BF)
        left[0, m] = nbv
        acc = xv
        for j in range(nt):
            cols = slice(j * tile, (j + 1) * tile)
            u = dot_nn(nbv, w[0, :, cols])
            uu = u * u
            bent = jnp.tanh(u * (gelu_coef + (gelu_coef * 0.044715) * uu))
            hu = 0.5 * u
            hp = 0.5 + 0.5 * bent
            hid = (u * hp).astype(BF)
            right[1, m, :, cols] = hid
            slope[m, :, cols] = hp + hu * (1.0 - bent * bent) * (
                gelu_coef + (gelu_coef * 3.0 * 0.044715) * uu
            )
            if second is not None:
                acc = acc + second(hid, cols)
        if second is not None:
            fout[m] = acc.astype(BF)

    slots = 2 * (ns - 1) + mb
    first_b = jnp.where(s == ns - 1, ns - 1, jnp.maximum(2 * (ns - 1) - s, s + mb - 1))

    def slot_of(*by_section):
        at_t = jnp.int32(min(by_section[-1], slots - 1))
        for sec, value in enumerate(by_section[:-1]):
            at_t = jnp.where(s == sec, min(value, slots - 1), at_t)
        return at_t

    t_near = slot_of(4, 5, 0, 0)
    t_next = slot_of(4, 5, 6, 6)
    t_last = slot_of(4, 6, 9, 7)
    t_far = slot_of(9, 9, 9, 8)
    t_shared = slot_of(5, 9, 9, 9)

    @pl.when(s == 0)
    def _():
        forward(0, lambda hid, cols: dot_nt(hid, w[1, :, cols]))

    pl.semaphore_wait(
        barrier, 2 + nz + jnp.where(s > 0, 1, 0) + jnp.where(s < ns - 1, 1, 0)
    )

    @pl.when(s == 0)
    def _():
        send_f(0).start()

    cp_mom.wait()
    for k in range(1, nz):
        g_z(k).start()
    cp_we.start()

    @pl.when(s > 0)
    def _():
        transposed(1)
        transposed(0)

    @pl.loop(0, slots)
    def _(t):
        mf = t - s
        mbk = t - first_b

        @pl.when(t == t_near)
        def _():
            from_z(0)

        @pl.when(t == t_next)
        def _():
            from_z(1)
            from_x(0)

        @pl.when(t == t_last)
        def _():
            from_x(1)

        @pl.when(t == t_far)
        def _():
            from_far()

        @pl.when(t == t_shared)
        def _():
            cp_we.wait()
            for j, q in enumerate((x, na, nb)):
                add_shared(q, j)
            flip(0)

        has_f = jnp.logical_and(mf >= 0, mf < mb)

        @pl.when(jnp.logical_and(jnp.logical_and(has_f, s == 0), t > 0))
        def _():
            forward(mf, lambda hid, cols: dot_nt(hid, w[1, :, cols]))

        @pl.when(jnp.logical_and(has_f, jnp.logical_and(s > 0, s < ns - 1)))
        def _():
            send_f(mf).wait_recv()
            forward(mf, lambda hid, cols: dot_nn(hid, wt[1, cols, :]))

        @pl.when(jnp.logical_and(jnp.logical_and(has_f, s < ns - 1), t > 0))
        def _():
            send_f(mf).start()

        @pl.when(jnp.logical_and(has_f, s == ns - 1))
        def _():
            send_f(mf).wait_recv()
            forward(mf, None)

        @pl.when(jnp.logical_and(mbk >= 0, mbk < mb))
        def _():
            @pl.when(s < ns - 1)
            def _():
                send_b(mbk).wait_recv()

            g = left[1, mbk]
            for j in range(nt):
                cols = slice(j * tile, (j + 1) * tile)
                bh = dot_nn(g, w[1, :, cols])
                right[0, mbk, :, cols] = (bh * slope[mbk, :, cols]).astype(BF)

            @pl.when(s > 0)
            def _():
                bn = dot_nn(right[0, mbk], wt[0])
                normed = nf[mbk]
                first = jnp.mean(bn, axis=-1, keepdims=True)
                second = jnp.mean(bn * normed, axis=-1, keepdims=True)
                sc = scf[mbk][:, :1]
                gout[mbk] = (g.astype(F32) + sc * (bn - first - normed * second)).astype(BF)
                send_b(mbk).start()

    cp_ow.wait()
    cp_var.wait()
    cp_se.wait()

    qx = NX // 2
    ct = 512 if hc % 512 == 0 else 256
    nct = hc // ct
    rows = qx * nz * NC * 16

    def first_pass(i, idx, sq):
        j = pl.multiple_of(idx * ct, ct)
        rt = right[i, :, :, pl.ds(j, ct)].reshape(mb * tok, ct)
        grad = dot_nn(lt[i], rt)
        c = comb[pl.ds(i * qx, qx), :, :, :, pl.ds(j, ct)].reshape(rows, ct) + 0.1 * grad
        comb[pl.ds(i * qx, qx), :, :, :, pl.ds(j, ct)] = c.reshape(qx, nz, NC, 16, ct)
        return sq + jnp.sum((c * c).reshape(rows // 8, 8, ct), axis=0)

    flip(1)
    late = opp // 2
    sq = lax.fori_loop(0, nct, functools.partial(first_pass, 1 - late), jnp.zeros((8, ct), F32))
    add_shared(opp, 3)
    sq = lax.fori_loop(0, nct, functools.partial(first_pass, late), sq)
    total_sq = jnp.sum(jnp.sum(sq, axis=0, keepdims=True), axis=1, keepdims=True)
    scale = jnp.sqrt(total_sq * (1.0 / (2 * d * hc)) + 0.01)
    inverse = 1.0 / scale

    quarters = (opp, na, nb, x)

    def slot_z(k):
        zeta = half + (k % 2) * ((k + 1) // 2 + k // 2) - k // 2
        return (z + zeta) % nz

    def to_partner(j, k):
        return remote(
            packed.at[quarters[j], slot_z(k), 1 - core], d0.at[j, k], d_s.at[j, k], d_r.at[j, k], partner
        )

    def second_pass(j, lo, hi):
        q = quarters[j]

        @pl.loop(lo, hi)
        def _(k):
            zz = slot_z(k)
            c = comb[q, zz].reshape(NC * 16, hc)
            p = (scale * jnp.tanh(c * inverse)).astype(BF)
            packed[q, zz] = p.reshape(NC, 16, hc)
            ne[q, zz] = (c - p.astype(F32)).astype(BF).reshape(NC, 16, hc)
            to_partner(j, k).start()

    def pair_sum(j, lo, hi):
        @pl.loop(lo, hi)
        def _(k):
            to_partner(j, k).wait_recv()
            s0[j, k] = (packed[quarters[j], slot_z(k), core].astype(F32) + d0[j, k].astype(F32)).astype(BF)

    def pack(p):
        for j in range(3):
            second_pass(j, 2 * p, 2 * p + 2)

    def sum_far(p):
        pair_sum(0, 2 * p, 2 * p + 2)
        far(p)

    def sum_near(p):
        pair_sum(1, 2 * p, 2 * p + 2)
        pair_sum(2, 2 * p, 2 * p + 2)

    def send_opp(g):
        to = dev_a if g % 2 == 0 else dev_b
        return remote(s0.at[0, g], ra.at[g], a_s.at[g], a_r.at[g], to)

    def send_a(g):
        return remote(s0.at[1, g], fa.at[g], ta_s.at[g], ta_r.at[g], dev_a)

    def send_bb(g):
        return remote(s0.at[2, g], fb.at[g], tb_s.at[g], tb_r.at[g], dev_b)

    def far(p):
        send_opp(2 * p).start()
        send_opp(2 * p + 1).start()

    def near(p):
        send_a(2 * p).start()
        send_bb(2 * p + 1).start()

    def augment(p):
        for g in (2 * p, 2 * p + 1):
            send_opp(g).wait_recv()
            slot = 2 if g % 2 == 0 else 1
            s0[slot, g] = (s0[slot, g].astype(F32) + ra[g].astype(F32)).astype(BF)
            (send_bb if slot == 2 else send_a)(g).start()

    def z_of(k):
        return (half + (k + 1) // 2 if k % 2 else half - k // 2) % nz

    def send_z(k):
        return remote(s1.at[k], zr.at[k], z_s.at[k], z_r.at[k], dev_z(z_of(k) if k else nz - 1))

    def along_z(p):
        for k in (2 * p, 2 * p + 1):
            send_a(k).wait_recv()
            send_bb(k).wait_recv()
            s1[k] = (s0[3, k].astype(F32) + fa[k].astype(F32) + fb[k].astype(F32)).astype(BF)
            if z_of(k) and k != 1:
                send_z(k).start()

    def relayed():
        send_z(0).wait_recv()
        s1[1] = (s1[1].astype(F32) + zr[0].astype(F32)).astype(BF)
        send_z(1).start()

    rounds = nz // 2
    pack(0)
    pack(1)
    sum_far(0)
    sum_near(0)
    near(0)
    sum_far(1)
    sum_near(1)
    for p in range(2, rounds):
        pack(p)
    second_pass(3, 0, nz)
    augment(0)
    near(1)
    if rounds > 2:
        sum_far(2)
        sum_near(2)
    pair_sum(3, 0, nz)
    augment(1)
    if rounds > 2:
        near(2)
        sum_far(3)
        sum_near(3)
        along_z(0)
        augment(2)
        near(3)
        along_z(1)
        relayed()
        augment(3)
        along_z(2)
        along_z(3)
    else:
        along_z(0)
        relayed()
        along_z(1)

    total = s1[nz - 1].astype(F32)
    for k in range(1, nz - 1):
        send_z(k).wait_recv()
        total = total + zr[k].astype(F32)
    merged = total * (1.0 / (NX * nz * NC)) + se[0]
    msq = jnp.sum(jnp.sum(merged * merged, axis=0, keepdims=True), axis=1, keepdims=True)
    sscale = jnp.sqrt(msq * (1.0 / (16 * hc)) + 0.01)
    values = (sscale * jnp.tanh(merged * (1.0 / sscale))).astype(BF)
    vf = values.astype(F32)
    nm_ref[0] = values
    nse_ref[0] = merged - vf
    step = 0.01 * vf / (jnp.sqrt(var[0].astype(F32)) + 1e-08)
    nw_ref[0] = (own_w[...].astype(F32) - step).astype(BF)

    for m in range(mb):
        @pl.when(s < ns - 1)
        def _():
            send_f(m).wait_send()

        @pl.when(s > 0)
        def _():
            send_b(m).wait_send()

    for k in range(1, nz):
        g_z(k).wait_send()
    for k in range(nz):
        g_x(x, k, 0).wait_send()
        g_x(x, k, 1).wait_send()
        g_y(nb if k % 2 == 0 else na, k).wait_send()
        for j, xx in enumerate((x, na, nb, opp)):
            g_d(j, xx, k, core).wait_send()
    for j in range(4):
        for k in range(nz):
            to_partner(j, k).wait_send()
    for g in range(nz):
        send_opp(g).wait_send()
        send_a(g).wait_send()
        send_bb(g).wait_send()
    for k in range(nz - 1):
        send_z(k).wait_send()


def store_kernel(a, b, c, e, a_out, b_out, c_out, e_out, sems):
    copies = [
        pltpu.make_async_copy(src, dst, sems.at[k])
        for k, (src, dst) in enumerate(((c, c_out), (e, e_out), (a, a_out), (b, b_out)))
    ]
    for copy in copies:
        copy.start()
    for copy in copies:
        copy.wait()


def local(ns, nz, token_ids, embed, weights, variance, momentum, worker_error, server_error, cotangent):
    mb, tok = token_ids.shape
    d = embed.shape[1]
    hc = weights.shape[3]
    dims = (NX, nz, NC, 16, hc)
    vm = pl.BlockSpec(memory_space=pltpu.VMEM)
    hbm = pl.BlockSpec(memory_space=pl.ANY)
    dma = pltpu.SemaphoreType.DMA
    tile = 1024 if hc % 512 == 0 else 128
    kernel = functools.partial(step_kernel, ns, nz, mb, tok, d, hc, tile)
    nw, nm, ne, nse = pl.pallas_call(
        kernel,
        out_shape=(
            pltpu.VMEM((1, 16, hc), BF),
            pltpu.VMEM((1, 16, hc), BF),
            pltpu.VMEM(dims, BF),
            pltpu.VMEM((1, 16, hc), F32),
        ),
        in_specs=[hbm] * 8,
        out_specs=(vm, vm, vm, vm),
        scratch_shapes=[
            pltpu.VMEM((mb, tok), jnp.int32),
            pltpu.VMEM(embed.shape, BF),
            pltpu.VMEM((1, 16, hc), BF),
            pltpu.VMEM((1, 16, hc), F32),
            pltpu.VMEM((2, d, hc), BF),
            pltpu.VMEM((2, hc, d), BF),
            pltpu.VMEM((16, hc), BF),
            pltpu.VMEM(dims, BF),
            pltpu.VMEM(dims, BF),
            pltpu.VMEM(dims, F32),
            pltpu.VMEM(dims, BF),
            pltpu.VMEM((mb, tok, d), BF),
            pltpu.VMEM((mb, tok, d), BF),
            pltpu.VMEM((mb, tok, d), BF),
            pltpu.VMEM((mb, tok, d), F32),
            pltpu.VMEM((mb, tok, 128), F32),
            pltpu.VMEM((mb, tok, hc), F32),
            pltpu.VMEM((2, mb, tok, d), BF),
            pltpu.VMEM((2, mb, tok, hc), BF),
            pltpu.VMEM((2, d, mb * tok), BF),
            pltpu.VMEM((4, nz, 16, hc), BF),
            pltpu.VMEM((4, nz, 16, hc), BF),
            pltpu.VMEM((nz, 16, hc), BF),
            pltpu.VMEM((nz, 16, hc), BF),
            pltpu.VMEM((nz, 16, hc), BF),
            pltpu.VMEM((nz, 16, hc), BF),
            pltpu.VMEM((nz, 16, hc), BF),
            dma((10,)),
            dma((mb,)), dma((mb,)), dma((mb,)), dma((mb,)),
            dma((nz,)), dma((nz,)), dma((2, nz)), dma((2, nz)), dma((nz,)), dma((nz,)), dma((4, nz)), dma((4, nz)),
            dma((4, nz)), dma((4, nz)), dma((nz,)), dma((nz,)), dma((nz,)), dma((nz,)), dma((nz,)), dma((nz,)),
            dma((nz,)), dma((nz,)),
        ],
        compiler_params=pltpu.CompilerParams(
            collective_id=0, has_side_effects=True, vmem_limit_bytes=48 * 1024 * 1024
        ),
        name="step",
    )(*(
        pltpu.with_memory_space_constraint(a, pltpu.MemorySpace.HBM)
        for a in (
            token_ids, embed, weights, variance, momentum,
            worker_error.reshape(dims), server_error, cotangent,
        )
    ))
    arrays = (nw, nm, ne, nse)
    nw, nm, ne, nse = pl.pallas_call(
        store_kernel,
        out_shape=tuple(jax.ShapeDtypeStruct(a.shape, a.dtype) for a in arrays),
        in_specs=[vm] * 4,
        out_specs=(hbm,) * 4,
        scratch_shapes=[dma((4,))],
        compiler_params=pltpu.CompilerParams(vmem_limit_bytes=4 * 1024 * 1024),
        name="store",
    )(*(pltpu.with_memory_space_constraint(a, pltpu.MemorySpace.VMEM) for a in arrays))
    return (nw, nm, ne.reshape(worker_error.shape), nse)


def solution(mesh):
    ns = mesh.shape["section"]
    nz = mesh.shape["dp"] // (NX * NC)
    in_specs = (
        P(None, "dp"),
        P(),
        P("section", None, None, None),
        P("section", "dp", None),
        P("section", "dp", None),
        P("section", "dp", None, None, None),
        P("section", "dp", None),
        P(None, "dp", None),
    )
    out_specs = (
        P("section", "dp", None),
        P("section", "dp", None),
        P("section", "dp", None, None, None),
        P("section", "dp", None),
    )
    return jax.shard_map(
        functools.partial(local, ns, nz), mesh=mesh, in_specs=in_specs, out_specs=out_specs,
        check_vma=False,
    )
```

```python
import functools
import math

import jax
import jax.numpy as jnp
from jax import lax
from jax.experimental import pallas as pl
from jax.experimental.pallas import tpu as pltpu
from jax.sharding import PartitionSpec as P

gelu_coef = math.sqrt(2.0 / math.pi)
MESH = pl.DeviceIdType.MESH
BF = jnp.bfloat16
F32 = jnp.float32
NX = 4
NC = 2


def dot_nn(a, b):
    return lax.dot_general(a, b, (((1,), (0,)), ((), ())), preferred_element_type=F32)


def dot_nt(a, b):
    return lax.dot_general(a, b, (((1,), (1,)), ((), ())), preferred_element_type=F32)


def dot_tn(a, b):
    return lax.dot_general(a, b, (((0,), (0,)), ((), ())), preferred_element_type=F32)


def step_kernel(
    ns, nz, mb, tok, d, hc, tile,
    ids_hbm, embed_hbm, w_hbm, var_hbm, mom_hbm, we_hbm, se_hbm, cot_hbm,
    nw_ref, nm_ref, ne, nse_ref,
    ids, embed, var, se, w, wt, own_w, we, mom, comb, packed, xin, fout, gout, nf, scf, slope, left, right, lt,
    d0, s0, ra, fa, fb, s1, zr,
    loc, f_s, f_r, b_s, b_r, gz_s, gz_r, gx_s, gx_r, gy_s, gy_r, gd_s, gd_r,
    d_s, d_r, a_s, a_r, ta_s, ta_r, tb_s, tb_r, z_s, z_r,
):
    s = lax.axis_index("section")
    r = lax.axis_index("dp")
    core = r % NC
    z = (r // NC) % nz
    x = r // (NC * nz)
    na = x + 1 - 2 * (x % 2)
    nb = 3 - x
    opp = (x + 2) % 4
    half = nz // 2

    def at(xx, zz, cc):
        return (xx * nz + zz) * NC + cc

    partner = at(x, z, 1 - core)
    dev_a = at(na, z, core)
    dev_b = at(nb, z, core)

    def dev_z(zeta):
        return at(x, (z + zeta) % nz, core)

    def remote(src, dst, send, recv, to):
        return pltpu.make_async_remote_copy(
            src_ref=src, dst_ref=dst, send_sem=send, recv_sem=recv,
            device_id={"dp": to}, device_id_type=MESH,
        )

    barrier = pltpu.get_barrier_semaphore()
    for peer in [partner, dev_a, dev_b] + [dev_z(k) for k in range(1, nz)]:
        pl.semaphore_signal(barrier, inc=1, device_id={"dp": peer}, device_id_type=MESH)

    @pl.when(s > 0)
    def _():
        pl.semaphore_signal(barrier, inc=1, device_id={"section": s - 1}, device_id_type=MESH)

    @pl.when(s < ns - 1)
    def _():
        pl.semaphore_signal(barrier, inc=1, device_id={"section": s + 1}, device_id_type=MESH)

    cp_mom = pltpu.make_async_copy(mom_hbm.at[0], mom.at[x, z, core], loc.at[0])
    cp_w0 = pltpu.make_async_copy(w_hbm.at[0, 0], w.at[0], loc.at[1])
    cp_w1 = pltpu.make_async_copy(w_hbm.at[0, 1], w.at[1], loc.at[2])
    cp_we = pltpu.make_async_copy(we_hbm, we, loc.at[3])
    cp_ow = pltpu.make_async_copy(
        w_hbm.at[0, x // 2, pl.ds(pl.multiple_of((r % (NC * nz * 2)) * 16, 16), 16)], own_w, loc.at[4]
    )
    cp_ids = pltpu.make_async_copy(ids_hbm, ids, loc.at[5])
    cp_embed = pltpu.make_async_copy(embed_hbm, embed, loc.at[6])
    cp_var = pltpu.make_async_copy(var_hbm, var, loc.at[7])
    cp_se = pltpu.make_async_copy(se_hbm, se, loc.at[8])
    cp_cot = pltpu.make_async_copy(cot_hbm, left.at[1], loc.at[9])
    @pl.when(s == 0)
    def _():
        cp_ids.start()
        cp_embed.start()

    cp_w0.start()
    cp_w1.start()
    cp_mom.start()

    @pl.when(s == ns - 1)
    def _():
        cp_cot.start()

    cp_ow.start()
    cp_var.start()
    cp_se.start()

    @pl.when(s == 0)
    def _():
        vocab = embed.shape[0]
        cp_ids.wait()
        cp_embed.wait()
        for m in range(mb):
            hot = (
                lax.broadcasted_iota(jnp.int32, (vocab, tok), 0) == ids[m : m + 1, :]
            ).astype(F32).astype(BF)
            xin[m] = dot_tn(hot, embed[...]).astype(BF)

    def transposed(i):
        step = 256 if hc % 256 == 0 else hc

        @pl.loop(0, hc // step)
        def _(j):
            lo = pl.multiple_of(j * step, step)
            wt[i, pl.ds(lo, step), :] = w[i, :, pl.ds(lo, step)].T

    @pl.when(s == ns - 1)
    def _():
        cp_cot.wait()

    cp_w0.wait()
    cp_w1.wait()

    order = [0]
    for dist in range(1, half):
        order += [dist, nz - dist]
    order.append(half)
    parts = (range(0, half + 1), range(half + 1, nz))

    def mom_at(xx, k):
        return mom.at[xx, (z + order[k]) % nz, core]

    def g_z(k):
        blk = mom.at[x, z, core]
        return remote(blk, blk, gz_s.at[k], gz_r.at[order.index((nz - order[k]) % nz)], dev_z(order[k]))

    def g_z_in(k):
        blk = mom_at(x, k)
        return remote(blk, blk, gz_s.at[k], gz_r.at[k], dev_z(order[k]))

    def g_x(xx, k, j):
        blk = mom_at(xx, k)
        return remote(blk, blk, gx_s.at[j, k], gx_r.at[j, k], (dev_a, dev_b)[j])

    def g_y(xx, k):
        blk = mom_at(xx, k)
        return remote(blk, blk, gy_s.at[k], gy_r.at[k], (dev_a, dev_b)[k % 2])

    def g_d(j, xx, k, cc):
        blk = mom.at[xx, (z + order[k]) % nz, cc]
        return remote(blk, blk, gd_s.at[j, k], gd_r.at[j, k], partner)

    def from_z(part):
        for k in parts[part]:
            if k:
                g_z_in(k).wait_recv()
            g_x(x, k, 0).start()
            g_x(x, k, 1).start()
            g_d(0, x, k, core).start()

    def from_x(part):
        for k in parts[part]:
            g_x(na, k, 0).wait_recv()
            g_x(nb, k, 1).wait_recv()
            g_y(nb if k % 2 == 0 else na, k).start()
            g_d(1, na, k, core).start()
            g_d(2, nb, k, core).start()

    def from_far():
        for k in range(nz):
            g_y(opp, k).wait_recv()
            g_d(3, opp, k, core).start()

    def add_shared(q, j):
        for k in range(nz):
            g_d(j, q, k, 1 - core).wait_recv()

        @pl.loop(0, nz)
        def _(k):
            comb[q, k] = 0.9 * mom[q, k].astype(F32) + we[q, k].astype(F32)

    def flip(i):
        lt[i] = left[i].reshape(mb * tok, d).T

    def send_f(m):
        return pltpu.make_async_remote_copy(
            src_ref=fout.at[m], dst_ref=xin.at[m], send_sem=f_s.at[m], recv_sem=f_r.at[m],
            device_id={"section": jnp.minimum(s + 1, ns - 1)}, device_id_type=MESH,
        )

    def send_b(m):
        return pltpu.make_async_remote_copy(
            src_ref=gout.at[m], dst_ref=left.at[1, m], send_sem=b_s.at[m], recv_sem=b_r.at[m],
            device_id={"section": jnp.maximum(s - 1, 0)}, device_id_type=MESH,
        )

    nt = hc // tile

    def forward(m, second):
        xv = xin[m].astype(F32)
        center = jnp.mean(xv, axis=-1, keepdims=True)
        dev = xv - center
        spread = jnp.mean(dev * dev, axis=-1, keepdims=True)
        scaled = lax.rsqrt(spread + 1e-05)
        normed = dev * scaled
        nf[m] = normed
        scf[m] = jnp.broadcast_to(scaled, (tok, 128))
        nbv = normed.astype(BF)
        left[0, m] = nbv
        acc = xv
        for j in range(nt):
            cols = slice(j * tile, (j + 1) * tile)
            u = dot_nn(nbv, w[0, :, cols])
            uu = u * u
            bent = jnp.tanh(u * (gelu_coef + (gelu_coef * 0.044715) * uu))
            hu = 0.5 * u
            hp = 0.5 + 0.5 * bent
            hid = (u * hp).astype(BF)
            right[1, m, :, cols] = hid
            slope[m, :, cols] = hp + hu * (1.0 - bent * bent) * (
                gelu_coef + (gelu_coef * 3.0 * 0.044715) * uu
            )
            if second is not None:
                acc = acc + second(hid, cols)
        if second is not None:
            fout[m] = acc.astype(BF)

    slots = 2 * (ns - 1) + mb
    first_b = jnp.where(s == ns - 1, ns - 1, jnp.maximum(2 * (ns - 1) - s, s + mb - 1))

    def slot_of(*by_section):
        at_t = jnp.int32(min(by_section[-1], slots - 1))
        for sec, value in enumerate(by_section[:-1]):
            at_t = jnp.where(s == sec, min(value, slots - 1), at_t)
        return at_t

    t_near = slot_of(4, 5, 0, 0)
    t_next = slot_of(4, 5, 6, 5)
    t_last = slot_of(4, 6, 8, 7)
    t_far = slot_of(7, 8, 9, 8)
    t_shared = slot_of(5, 9, 9, 9)

    @pl.when(s == 0)
    def _():
        forward(0, lambda hid, cols: dot_nt(hid, w[1, :, cols]))

    pl.semaphore_wait(
        barrier, 2 + nz + jnp.where(s > 0, 1, 0) + jnp.where(s < ns - 1, 1, 0)
    )

    @pl.when(s == 0)
    def _():
        send_f(0).start()

    cp_mom.wait()
    for k in range(1, nz):
        g_z(k).start()
    cp_we.start()

    @pl.when(s > 0)
    def _():
        transposed(1)
        transposed(0)

    @pl.loop(0, slots)
    def _(t):
        mf = t - s
        mbk = t - first_b

        @pl.when(t == t_near)
        def _():
            from_z(0)

        @pl.when(t == t_next)
        def _():
            from_z(1)
            from_x(0)

        @pl.when(t == t_last)
        def _():
            from_x(1)

        @pl.when(t == t_far)
        def _():
            from_far()

        @pl.when(t == t_shared)
        def _():
            cp_we.wait()
            for j, q in enumerate((x, na, nb)):
                add_shared(q, j)
            flip(0)

        @pl.when(t == slots - 1)
        def _():
            add_shared(opp, 3)

        has_f = jnp.logical_and(mf >= 0, mf < mb)

        @pl.when(jnp.logical_and(jnp.logical_and(has_f, s == 0), t > 0))
        def _():
            forward(mf, lambda hid, cols: dot_nt(hid, w[1, :, cols]))

        @pl.when(jnp.logical_and(has_f, jnp.logical_and(s > 0, s < ns - 1)))
        def _():
            send_f(mf).wait_recv()
            forward(mf, lambda hid, cols: dot_nn(hid, wt[1, cols, :]))

        @pl.when(jnp.logical_and(jnp.logical_and(has_f, s < ns - 1), t > 0))
        def _():
            send_f(mf).start()

        @pl.when(jnp.logical_and(has_f, s == ns - 1))
        def _():
            send_f(mf).wait_recv()
            forward(mf, None)

        @pl.when(jnp.logical_and(mbk >= 0, mbk < mb))
        def _():
            @pl.when(s < ns - 1)
            def _():
                send_b(mbk).wait_recv()

            g = left[1, mbk]
            for j in range(nt):
                cols = slice(j * tile, (j + 1) * tile)
                bh = dot_nn(g, w[1, :, cols])
                right[0, mbk, :, cols] = (bh * slope[mbk, :, cols]).astype(BF)

            @pl.when(s > 0)
            def _():
                bn = dot_nn(right[0, mbk], wt[0])
                normed = nf[mbk]
                first = jnp.mean(bn, axis=-1, keepdims=True)
                second = jnp.mean(bn * normed, axis=-1, keepdims=True)
                sc = scf[mbk][:, :1]
                gout[mbk] = (g.astype(F32) + sc * (bn - first - normed * second)).astype(BF)
                send_b(mbk).start()

    cp_ow.wait()
    cp_var.wait()
    cp_se.wait()

    qx = NX // 2
    ct = 1024 if hc % 1024 == 0 else 256
    nct = hc // ct
    rows = qx * nz * NC * 16

    def first_pass(idx, sq):
        i = idx // nct
        j = pl.multiple_of((idx % nct) * ct, ct)
        rt = right[i, :, :, pl.ds(j, ct)].reshape(mb * tok, ct)
        grad = dot_nn(lt[i], rt)
        c = comb[pl.ds(i * qx, qx), :, :, :, pl.ds(j, ct)].reshape(rows, ct) + 0.1 * grad
        comb[pl.ds(i * qx, qx), :, :, :, pl.ds(j, ct)] = c.reshape(qx, nz, NC, 16, ct)
        return sq + jnp.sum((c * c).reshape(rows // 8, 8, ct), axis=0)

    flip(1)
    sq = lax.fori_loop(0, 2 * nct, first_pass, jnp.zeros((8, ct), F32))
    total_sq = jnp.sum(jnp.sum(sq, axis=0, keepdims=True), axis=1, keepdims=True)
    scale = jnp.sqrt(total_sq * (1.0 / (2 * d * hc)) + 0.01)
    inverse = 1.0 / scale

    quarters = (opp, na, nb, x)

    def slot_z(k):
        zeta = half + (k % 2) * ((k + 1) // 2 + k // 2) - k // 2
        return (z + zeta) % nz

    def to_partner(j, k):
        return remote(
            packed.at[quarters[j], slot_z(k), 1 - core], d0.at[j, k], d_s.at[j, k], d_r.at[j, k], partner
        )

    def second_pass(j, lo, hi):
        q = quarters[j]

        @pl.loop(lo, hi)
        def _(k):
            zz = slot_z(k)
            c = comb[q, zz].reshape(NC * 16, hc)
            p = (scale * jnp.tanh(c * inverse)).astype(BF)
            packed[q, zz] = p.reshape(NC, 16, hc)
            ne[q, zz] = (c - p.astype(F32)).astype(BF).reshape(NC, 16, hc)
            to_partner(j, k).start()

    def pair_sum(j, lo, hi):
        @pl.loop(lo, hi)
        def _(k):
            to_partner(j, k).wait_recv()
            s0[j, k] = (packed[quarters[j], slot_z(k), core].astype(F32) + d0[j, k].astype(F32)).astype(BF)

    def pack(p):
        for j in range(3):
            second_pass(j, 2 * p, 2 * p + 2)

    def sum_far(p):
        pair_sum(0, 2 * p, 2 * p + 2)
        far(p)

    def sum_near(p):
        pair_sum(1, 2 * p, 2 * p + 2)
        pair_sum(2, 2 * p, 2 * p + 2)

    def send_opp(g):
        to = dev_a if g % 2 == 0 else dev_b
        return remote(s0.at[0, g], ra.at[g], a_s.at[g], a_r.at[g], to)

    def send_a(g):
        return remote(s0.at[1, g], fa.at[g], ta_s.at[g], ta_r.at[g], dev_a)

    def send_bb(g):
        return remote(s0.at[2, g], fb.at[g], tb_s.at[g], tb_r.at[g], dev_b)

    def far(p):
        send_opp(2 * p).start()
        send_opp(2 * p + 1).start()

    def near(p):
        send_a(2 * p).start()
        send_bb(2 * p + 1).start()

    def augment(p):
        for g in (2 * p, 2 * p + 1):
            send_opp(g).wait_recv()
            slot = 2 if g % 2 == 0 else 1
            s0[slot, g] = (s0[slot, g].astype(F32) + ra[g].astype(F32)).astype(BF)
            (send_bb if slot == 2 else send_a)(g).start()

    def z_of(k):
        return (half + (k + 1) // 2 if k % 2 else half - k // 2) % nz

    def send_z(k):
        return remote(s1.at[k], zr.at[k], z_s.at[k], z_r.at[k], dev_z(z_of(k) if k else nz - 1))

    def along_z(p):
        for k in (2 * p, 2 * p + 1):
            send_a(k).wait_recv()
            send_bb(k).wait_recv()
            s1[k] = (s0[3, k].astype(F32) + fa[k].astype(F32) + fb[k].astype(F32)).astype(BF)
            if z_of(k) and k != 1:
                send_z(k).start()

    def relayed():
        send_z(0).wait_recv()
        s1[1] = (s1[1].astype(F32) + zr[0].astype(F32)).astype(BF)
        send_z(1).start()

    rounds = nz // 2
    pack(0)
    pack(1)
    sum_far(0)
    sum_near(0)
    near(0)
    sum_far(1)
    sum_near(1)
    for p in range(2, rounds):
        pack(p)
    second_pass(3, 0, nz)
    augment(0)
    near(1)
    if rounds > 2:
        sum_far(2)
        sum_near(2)
    pair_sum(3, 0, nz)
    augment(1)
    if rounds > 2:
        near(2)
        sum_far(3)
        sum_near(3)
        along_z(0)
        augment(2)
        near(3)
        along_z(1)
        relayed()
        augment(3)
        along_z(2)
        along_z(3)
    else:
        along_z(0)
        relayed()
        along_z(1)

    total = s1[nz - 1].astype(F32)
    for k in range(1, nz - 1):
        send_z(k).wait_recv()
        total = total + zr[k].astype(F32)
    merged = total * (1.0 / (NX * nz * NC)) + se[0]
    msq = jnp.sum(jnp.sum(merged * merged, axis=0, keepdims=True), axis=1, keepdims=True)
    sscale = jnp.sqrt(msq * (1.0 / (16 * hc)) + 0.01)
    values = (sscale * jnp.tanh(merged * (1.0 / sscale))).astype(BF)
    vf = values.astype(F32)
    nm_ref[0] = values
    nse_ref[0] = merged - vf
    step = 0.01 * vf / (jnp.sqrt(var[0].astype(F32)) + 1e-08)
    nw_ref[0] = (own_w[...].astype(F32) - step).astype(BF)

    for m in range(mb):
        @pl.when(s < ns - 1)
        def _():
            send_f(m).wait_send()

        @pl.when(s > 0)
        def _():
            send_b(m).wait_send()

    for k in range(1, nz):
        g_z(k).wait_send()
    for k in range(nz):
        g_x(x, k, 0).wait_send()
        g_x(x, k, 1).wait_send()
        g_y(nb if k % 2 == 0 else na, k).wait_send()
        for j, xx in enumerate((x, na, nb, opp)):
            g_d(j, xx, k, core).wait_send()
    for j in range(4):
        for k in range(nz):
            to_partner(j, k).wait_send()
    for g in range(nz):
        send_opp(g).wait_send()
        send_a(g).wait_send()
        send_bb(g).wait_send()
    for k in range(nz - 1):
        send_z(k).wait_send()


def store_kernel(a, b, c, e, a_out, b_out, c_out, e_out, sems):
    copies = [
        pltpu.make_async_copy(src, dst, sems.at[k])
        for k, (src, dst) in enumerate(((c, c_out), (e, e_out), (a, a_out), (b, b_out)))
    ]
    for copy in copies:
        copy.start()
    for copy in copies:
        copy.wait()


def local(ns, nz, token_ids, embed, weights, variance, momentum, worker_error, server_error, cotangent):
    mb, tok = token_ids.shape
    d = embed.shape[1]
    hc = weights.shape[3]
    dims = (NX, nz, NC, 16, hc)
    vm = pl.BlockSpec(memory_space=pltpu.VMEM)
    hbm = pl.BlockSpec(memory_space=pl.ANY)
    dma = pltpu.SemaphoreType.DMA
    tile = 1024 if hc % 512 == 0 else 128
    kernel = functools.partial(step_kernel, ns, nz, mb, tok, d, hc, tile)
    nw, nm, ne, nse = pl.pallas_call(
        kernel,
        out_shape=(
            pltpu.VMEM((1, 16, hc), BF),
            pltpu.VMEM((1, 16, hc), BF),
            pltpu.VMEM(dims, BF),
            pltpu.VMEM((1, 16, hc), F32),
        ),
        in_specs=[hbm] * 8,
        out_specs=(vm, vm, vm, vm),
        scratch_shapes=[
            pltpu.VMEM((mb, tok), jnp.int32),
            pltpu.VMEM(embed.shape, BF),
            pltpu.VMEM((1, 16, hc), BF),
            pltpu.VMEM((1, 16, hc), F32),
            pltpu.VMEM((2, d, hc), BF),
            pltpu.VMEM((2, hc, d), BF),
            pltpu.VMEM((16, hc), BF),
            pltpu.VMEM(dims, BF),
            pltpu.VMEM(dims, BF),
            pltpu.VMEM(dims, F32),
            pltpu.VMEM(dims, BF),
            pltpu.VMEM((mb, tok, d), BF),
            pltpu.VMEM((mb, tok, d), BF),
            pltpu.VMEM((mb, tok, d), BF),
            pltpu.VMEM((mb, tok, d), F32),
            pltpu.VMEM((mb, tok, 128), F32),
            pltpu.VMEM((mb, tok, hc), F32),
            pltpu.VMEM((2, mb, tok, d), BF),
            pltpu.VMEM((2, mb, tok, hc), BF),
            pltpu.VMEM((2, d, mb * tok), BF),
            pltpu.VMEM((4, nz, 16, hc), BF),
            pltpu.VMEM((4, nz, 16, hc), BF),
            pltpu.VMEM((nz, 16, hc), BF),
            pltpu.VMEM((nz, 16, hc), BF),
            pltpu.VMEM((nz, 16, hc), BF),
            pltpu.VMEM((nz, 16, hc), BF),
            pltpu.VMEM((nz, 16, hc), BF),
            dma((10,)),
            dma((mb,)), dma((mb,)), dma((mb,)), dma((mb,)),
            dma((nz,)), dma((nz,)), dma((2, nz)), dma((2, nz)), dma((nz,)), dma((nz,)), dma((4, nz)), dma((4, nz)),
            dma((4, nz)), dma((4, nz)), dma((nz,)), dma((nz,)), dma((nz,)), dma((nz,)), dma((nz,)), dma((nz,)),
            dma((nz,)), dma((nz,)),
        ],
        compiler_params=pltpu.CompilerParams(
            collective_id=0, has_side_effects=True, vmem_limit_bytes=48 * 1024 * 1024
        ),
        name="step",
    )(*(
        pltpu.with_memory_space_constraint(a, pltpu.MemorySpace.HBM)
        for a in (
            token_ids, embed, weights, variance, momentum,
            worker_error.reshape(dims), server_error, cotangent,
        )
    ))
    arrays = (nw, nm, ne, nse)
    nw, nm, ne, nse = pl.pallas_call(
        store_kernel,
        out_shape=tuple(jax.ShapeDtypeStruct(a.shape, a.dtype) for a in arrays),
        in_specs=[vm] * 4,
        out_specs=(hbm,) * 4,
        scratch_shapes=[dma((4,))],
        compiler_params=pltpu.CompilerParams(vmem_limit_bytes=4 * 1024 * 1024),
        name="store",
    )(*(pltpu.with_memory_space_constraint(a, pltpu.MemorySpace.VMEM) for a in arrays))
    return (nw, nm, ne.reshape(worker_error.shape), nse)


def solution(mesh):
    ns = mesh.shape["section"]
    nz = mesh.shape["dp"] // (NX * NC)
    in_specs = (
        P(None, "dp"),
        P(),
        P("section", None, None, None),
        P("section", "dp", None),
        P("section", "dp", None),
        P("section", "dp", None, None, None),
        P("section", "dp", None),
        P(None, "dp", None),
    )
    out_specs = (
        P("section", "dp", None),
        P("section", "dp", None),
        P("section", "dp", None, None, None),
        P("section", "dp", None),
    )
    return jax.shard_map(
        functools.partial(local, ns, nz), mesh=mesh, in_specs=in_specs, out_specs=out_specs,
        check_vma=False,
    )
```
